8 devices in a mesh: rep: 2 (over y, z), dp: 4 (over x, core).
Axes of the slice: x: 2, y: 2, z: 1, core: 2. Of those that a mesh axis runs over, the one named last changes fastest.
Arguments:
- x: bfloat16 [8, 2048, 896], P(('rep', 'dp')), parts along dimension 0
- dy: bfloat16 [8, 2048, 896], P(('rep', 'dp')), parts along dimension 0
- w_gate: bfloat16 [2, 896, 2560], replicated
- w_up: bfloat16 [2, 896, 2560], replicated
- w_down: bfloat16 [2, 2560, 896], replicated
- m_w_gate: float32 [2, 896, 2560], P(None, 'dp')
- m_w_up: float32 [2, 896, 2560], P(None, 'dp')
- m_w_down: float32 [2, 2560, 896], P(None, 'dp')
- v_w_gate: float32 [2, 896, 2560], P(None, 'dp')
- v_w_up: float32 [2, 896, 2560], P(None, 'dp')
- v_w_down: float32 [2, 2560, 896], P(None, 'dp')
Outputs:
- output 1: bfloat16 [4, 896, 2560], P('rep'), parts along dimension 0
- output 2: bfloat16 [4, 896, 2560], P('rep'), parts along dimension 0
- output 3: bfloat16 [4, 2560, 896], P('rep'), parts along dimension 0
- output 4: float32 [4, 896, 2560], P('rep', 'dp'), parts along dimension 0
- output 5: float32 [4, 896, 2560], P('rep', 'dp'), parts along dimension 0
- output 6: float32 [4, 2560, 896], P('rep', 'dp'), parts along dimension 0
- output 7: float32 [4, 896, 2560], P('rep', 'dp'), parts along dimension 0
- output 8: float32 [4, 896, 2560], P('rep', 'dp'), parts along dimension 0
- output 9: float32 [4, 2560, 896], P('rep', 'dp'), parts along dimension 0
There are 2 independent parts. The reference program is written for one: setup_inputs(seed, part) draws one part's arguments, and reference() takes and returns one part's arrays. A program takes and returns all parts, laid end to end along the dimension named above; an argument that names none is the same for every part.
All inputs are finite; a program needn't handle non-finite values.
Results may differ from the reference program's by a relative error of at most 0.022.
Values are sent between devices in bfloat16 or wider.
A program may use at most 2 GiB of HBM per device.

```python
import jax
import jax.numpy as jnp
from jax import lax

SEQUENCES = 4
TOKENS = 2048
D = 896
FF = 2560
LAYERS = 2
NAMES = ("w_gate", "w_up", "w_down")
SHAPES = {"w_gate": (LAYERS, D, FF), "w_up": (LAYERS, D, FF), "w_down": (LAYERS, FF, D)}


def bump(key, n, height):
    away = (jnp.arange(n, dtype=jnp.int32) - jax.random.randint(key, (), 0, n, jnp.int32)) % n
    return jnp.where(away < n // 8, height, 1.0)


def together(key, own, strength):
    shared = jax.random.normal(key, own.shape[1:], jnp.float32)
    return (own + strength * shared) * lax.rsqrt(1 + strength * strength)


def setup_inputs(seed: int = 0, part: int = 0) -> dict:
    kx, kdy, ka, kb, kz, kf, kh, kl, *keys = jax.random.split(jax.random.key(seed), 8 + 3 * len(NAMES))
    kx, kdy, ka, kb = (jax.random.fold_in(k, part) for k in (kx, kdy, ka, kb))
    kw, km, kv = (keys[i::3] for i in range(3))
    shape = (SEQUENCES, TOKENS, D)
    much_x, much_dy = jax.random.uniform(kz, (2,), jnp.float32, 0.0, 1.0)
    loud = 2.0 ** jax.random.uniform(jax.random.fold_in(kz, 1), (), jnp.float32, -1.0, 2.0)
    layers = 2.0 ** jax.random.uniform(kl, (LAYERS, 1, 1), jnp.float32, -1.0, 1.0)
    x = together(ka, jax.random.normal(kx, shape, jnp.float32), much_x) * bump(kf, D, 4.0)
    dy = together(kb, jax.random.normal(kdy, shape, jnp.float32), much_dy)
    drawn = {"x": x.astype(jnp.bfloat16), "dy": (loud * dy * (SEQUENCES * TOKENS) ** -0.5).astype(jnp.bfloat16)}
    for key, name in zip(kw, NAMES, strict=True):
        w = jax.random.normal(key, SHAPES[name], jnp.float32) * SHAPES[name][1] ** -0.5
        drawn[name] = (w * {"w_gate": 1.0, "w_up": bump(kh, FF, 4.0), "w_down": layers}[name]).astype(jnp.bfloat16)
    for key, name in zip(km, NAMES, strict=True):
        drawn[f"m_{name}"] = 0.1 * jax.random.normal(key, SHAPES[name], jnp.float32)
    for key, name in zip(kv, NAMES, strict=True):
        drawn[f"v_{name}"] = jax.random.uniform(key, SHAPES[name], jnp.float32, 0.005, 0.015)
    return drawn


def matmul(a, w):
    return jnp.dot(a, w, preferred_element_type=jnp.float32).astype(jnp.bfloat16)


def normed(h):
    wide = h.astype(jnp.float32)
    scale = lax.rsqrt(jnp.mean(wide**2, -1, keepdims=True) + 1e-6)
    return (wide * scale).astype(jnp.bfloat16)


def layer(h, w):
    a = normed(h)
    gate = jnp.dot(a, w["w_gate"], preferred_element_type=jnp.float32)
    up = jnp.dot(a, w["w_up"], preferred_element_type=jnp.float32)
    return h + matmul((jax.nn.silu(gate) * up).astype(jnp.bfloat16), w["w_down"])


def adamw(w, m, v, g):
    m = 0.9 * m + 0.1 * g
    v = 0.95 * v + 0.05 * g * g
    step = m * lax.rsqrt(v + 1e-8) + 0.1 * w
    return (w - 0.02 * step).astype(jnp.bfloat16), m, v


def clipped(gradients, sum_of_squares, count):
    factor = jnp.minimum(1.0, 0.5 * lax.rsqrt(sum_of_squares / count + 1e-30))
    return [g * factor for g in gradients]


def stack(weights, h):
    return lax.scan(lambda h, w: (layer(h, w), None), h, weights)[0]


def reference(x, dy, w_gate, w_up, w_down, m_w_gate, m_w_up, m_w_down, v_w_gate, v_w_up, v_w_down):
    weights = dict(zip(NAMES, (w_gate, w_up, w_down), strict=True))

    def take(so_far, sequence):
        h, by_y = sequence
        _, back = jax.vjp(lambda w: stack(w, h), weights)
        return jax.tree.map(lambda total, term: total + term.astype(jnp.float32), so_far, back(by_y)[0]), None

    none_yet = {name: jnp.zeros(w.shape, jnp.float32) for name, w in weights.items()}
    by_weights, _ = lax.scan(take, none_yet, (x, dy))
    gradients = [by_weights[name].astype(jnp.bfloat16).astype(jnp.float32) for name in NAMES]
    gradients = clipped(gradients, sum(jnp.sum(g * g) for g in gradients), sum(g.size for g in gradients))
    new = [
        adamw(w.astype(jnp.float32), m, v, g)
        for w, m, v, g in zip((w_gate, w_up, w_down), (m_w_gate, m_w_up, m_w_down), (v_w_gate, v_w_up, v_w_down), gradients, strict=True)
    ]
    return tuple(one[which] for which in range(3) for one in new)
```

```python
import jax
import jax.numpy as jnp
from jax import lax
from jax.experimental import pallas as pl
from jax.experimental.pallas import tpu as pltpu
from jax.sharding import PartitionSpec as P

T, D, FF = 2048, 896, 2560
GROUP = 4
OWN_D, OWN_F = D // GROUP, FF // GROUP
CHUNKS, PIECE = 5, 128
C = GROUP * PIECE
TILE = 512
TILES = T // TILE
BF, F32 = jnp.bfloat16, jnp.float32
ANY = pl.BlockSpec(memory_space=pl.ANY)


def dot(a, b, over=(1, 0)):
    return lax.dot_general(a, b, (((over[0],), (over[1],)), ((), ())), preferred_element_type=F32)


def logistic(x):
    return 1.0 / (1.0 + jnp.exp(-x))


def normed(h):
    wide = h.astype(F32)
    return (wide * lax.rsqrt(jnp.mean(wide * wide, -1, keepdims=True) + 1e-6)).astype(BF)


def at(i, size):
    return pl.ds(pl.multiple_of(i * size, size), size)


def hidden(d, k):
    return pl.ds(pl.multiple_of(d * OWN_F + k * PIECE, PIECE), PIECE)


def forward_kernel(x, wg, wu, wd, s_out, q_out, p_out, h_out, a_out, at_out, a0t_out, wgs, wus, wds, p, sem):
    t = pl.program_id(0)

    def copies(k):
        for d in range(GROUP):
            yield pltpu.make_async_copy(wg.at[0, :, hidden(d, k)], wgs.at[k, :, at(d, PIECE)], sem.at[k, d])
            yield pltpu.make_async_copy(wu.at[0, :, hidden(d, k)], wus.at[k, :, at(d, PIECE)], sem.at[k, 4 + d])
        for d in range(GROUP):
            yield pltpu.make_async_copy(wd.at[0, hidden(d, k), :], wds.at[at(k * GROUP + d, PIECE), :], sem.at[k, 8 + d])

    @pl.when(t == 0)
    def _():
        @pl.loop(0, CHUNKS)
        def _(k):
            for c in copies(k):
                c.start()

    a = normed(x[0])
    a0t_out[...] = a.T

    @pl.loop(0, CHUNKS)
    def _(k):
        @pl.when(t == 0)
        def _():
            for c in copies(k):
                c.wait()

        gate = dot(a, wgs[k])
        up = dot(a, wus[k])
        s = logistic(gate)
        silu = gate * s
        prod = (silu * up).astype(BF)
        s_out[k] = silu
        q_out[k] = up * (s * (1.0 + gate * (1.0 - s)))
        p_out[k] = prod
        p[:, at(k, C)] = prod

    h = (x[0].astype(F32) + dot(p[...], wds[...]).astype(BF).astype(F32)).astype(BF)
    h_out[...] = h
    a = normed(h)
    a_out[...] = a
    at_out[...] = a.T


def forward(x, wg, wu, wd):
    wide = jax.ShapeDtypeStruct((CHUNKS, T, C), F32)
    rows = jax.ShapeDtypeStruct((T, D), BF)
    turned = jax.ShapeDtypeStruct((D, T), BF)
    block = pl.BlockSpec((CHUNKS, TILE, C), lambda t: (0, t, 0))
    row_block = pl.BlockSpec((TILE, D), lambda t: (t, 0))
    turned_block = pl.BlockSpec((D, TILE), lambda t: (0, t))
    return pl.pallas_call(
        forward_kernel,
        grid=(TILES,),
        out_shape=[wide, wide, jax.ShapeDtypeStruct((CHUNKS, T, C), BF), rows, rows, turned, turned],
        in_specs=[pl.BlockSpec((1, TILE, D), lambda t: (0, t, 0)), ANY, ANY, ANY],
        out_specs=[block, block, block, row_block, row_block, turned_block, turned_block],
        scratch_shapes=[
            pltpu.VMEM((CHUNKS, D, C), BF),
            pltpu.VMEM((CHUNKS, D, C), BF),
            pltpu.VMEM((FF, D), BF),
            pltpu.VMEM((TILE, FF), BF),
            pltpu.SemaphoreType.DMA((CHUNKS, 12)),
        ],
        compiler_params=pltpu.CompilerParams(vmem_limit_bytes=64_000_000),
        cost_estimate=pl.CostEstimate(flops=6 * T * D * FF, bytes_accessed=80_000_000, transcendentals=T * FF),
        name="forward",
    )(x, wg, wu, wd)


def backward_kernel(
    a1, a1t, dy, h1, a0t, s0, q0, p0, wg, wu, wd,
    gg, gu, gd, ss,
    a, atr, dh, h, pr, dg, du, da, wgv, wuv, wdv, dwg, dwd, rdg, rdd, isg, isd, irg, ird, owng, ownd, ssg, ssd, nsend, nrecv,
    isem, wsem, psem, ssem, d2d_send, d2d_recv, ici_send, ici_recv, osem, n_send, n_recv,
):
    me = lax.axis_index("dp")
    core, chip = me % 2, me // 2
    other = 1 - chip
    near, far, across = me + 1 - 2 * core, (me + 2) % 4, 3 - me

    def remote(src, dst, send, recv, to):
        return pltpu.make_async_remote_copy(src, dst, send, recv, device_id={"dp": to}, device_id_type=pl.DeviceIdType.MESH)

    def weights(layer, k, slot, all_three):
        for d in range(GROUP):
            yield pltpu.make_async_copy(wd.at[layer, hidden(d, k), :], wdv.at[slot, at(d, PIECE), :], wsem.at[slot, d])
        if all_three:
            for d in range(GROUP):
                yield pltpu.make_async_copy(wg.at[layer, :, hidden(d, k)], wgv.at[slot, :, at(d, PIECE)], wsem.at[slot, 4 + d])
                yield pltpu.make_async_copy(wu.at[layer, :, hidden(d, k)], wuv.at[slot, :, at(d, PIECE)], wsem.at[slot, 8 + d])

    def start(copies):
        for c in copies:
            c.start()

    def wait(copies):
        for c in copies:
            c.wait()

    def rows_of(k):
        return [pltpu.make_async_copy(p0.at[k], pr.at[(k + 1) % 2], psem.at[(k + 1) % 2])]

    def saved(step):
        k, t, slot = step // TILES, step % TILES, step % 2
        for i, source in enumerate((s0, q0)):
            yield pltpu.make_async_copy(source.at[k, at(t, TILE), :], da.at[at(2 * i + slot, TILE), pl.ds(0, C)], ssem.at[slot, i])

    first = [pltpu.make_async_copy(src, dst, isem.at[i]) for i, (src, dst) in enumerate(((a1, a), (dy, dh), (a1t, atr), (h1, h)))]
    start(weights(1, 0, 0, True))
    start(first)
    start(rows_of(0))
    barrier = pltpu.get_barrier_semaphore()
    for to in (near, far, across):
        pl.semaphore_signal(barrier, inc=1, device_id={"dp": to}, device_id_type=pl.DeviceIdType.MESH)
    ssg[...] = jnp.zeros_like(ssg)
    ssd[...] = jnp.zeros_like(ssd)

    @pl.loop(0, TILES)
    def _(t):
        da[at(t, TILE), :] = jnp.zeros((TILE, D), F32)

    pl.semaphore_wait(barrier, 3)
    wait(first)

    def weight_gradients(slot):
        @pl.loop(0, 2)
        def _(half):
            down = dot(pr[slot, :, at(half, 2 * PIECE)], dh[...], (0, 0)).astype(BF)
            dwd[1 - core, half] = down[:PIECE]
            dwd[core, half] = down[PIECE:]
            turned = atr[at(half, 2 * OWN_D), :]
            for i, d in enumerate((dg, du)):
                out = dot(turned, d[...]).astype(BF)
                rows = slice(i * OWN_D, (i + 1) * OWN_D)
                dwg[1 - core, half, rows, :] = out[:OWN_D]
                dwg[core, half, rows, :] = out[OWN_D:]

    def to_near(n):
        return [
            remote(dwd.at[0], rdd.at[n % 2], d2d_send.at[0, n], d2d_recv.at[0, n], near),
            remote(dwg.at[0], rdg.at[n % 2], d2d_send.at[1, n], d2d_recv.at[1, n], near),
        ]

    def to_far(n):
        return [
            remote(isd.at[n % CHUNKS], ird.at[n], ici_send.at[0, n], ici_recv.at[0, n], far),
            remote(isg.at[n % CHUNKS], irg.at[n], ici_send.at[1, n], ici_recv.at[1, n], far),
        ]

    def sum_on_chip(n):
        slot, place = n % 2, n % CHUNKS
        near_copies, far_copies = to_near(n), to_far(n)
        for own, got, out, near_copy, far_copy in ((dwd, rdd, isd, near_copies[0], far_copies[0]), (dwg, rdg, isg, near_copies[1], far_copies[1])):
            near_copy.wait()
            out[place] = (own[1, other].astype(F32) + got[slot, other].astype(F32)).astype(BF)
            far_copy.start()
        ownd[place] = dwd[1, chip].astype(F32) + rdd[slot, chip].astype(F32)
        owng[place] = dwg[1, chip].astype(F32) + rdg[slot, chip].astype(F32)

    def results(n, layer, k):
        yield pltpu.make_async_copy(ird.at[n], gd.at[layer, at(k, PIECE), :], osem.at[n, 0])
        for i, out in enumerate((gg, gu)):
            for d in range(GROUP):
                yield pltpu.make_async_copy(
                    irg.at[n, pl.ds(i * OWN_D, OWN_D), at(d, PIECE)], out.at[layer, :, hidden(d, k)], osem.at[n, 1 + i * GROUP + d]
                )

    def finish(n, layer, k):
        place = n % CHUNKS
        for own, got, total, copy in ((ownd, ird, ssd, to_far(n)[0]), (owng, irg, ssg, to_far(n)[1])):
            copy.wait()
            g = (own[place] + got[n].astype(F32)).astype(BF)
            got[n] = g
            g = g.astype(F32)
            total[...] += jnp.sum((g * g).reshape(-1, 8, g.shape[-1]), 0)
        start(results(n, layer, k))

    @pl.loop(0, CHUNKS)
    def _(k):
        slot = k % 2
        wait(weights(1, k, slot, True))

        @pl.when(k < CHUNKS - 1)
        def _():
            start(weights(1, k + 1, 1 - slot, True))

        @pl.when(k == CHUNKS - 1)
        def _():
            start(weights(0, 0, CHUNKS % 2, False))

        @pl.loop(0, TILES)
        def _(t):
            r = at(t, TILE)
            x = a[r, :]
            gate = dot(x, wgv[slot])
            up = dot(x, wuv[slot])
            dp = dot(dh[r, :], wdv[slot], (1, 1)).astype(BF).astype(F32)
            s = logistic(gate)
            silu = gate * s
            pr[0, r, :] = (silu * up).astype(BF)
            dg[r, :] = (dp * (up * (s * (1.0 + gate * (1.0 - s))))).astype(BF)
            du[r, :] = (dp * silu).astype(BF)

        weight_gradients(0)
        start(to_near(k))

        @pl.loop(0, TILES)
        def _(t):
            r = at(t, TILE)
            da[r, :] += dot(dg[r, :], wgv[slot], (1, 1)) + dot(du[r, :], wuv[slot], (1, 1))

        sum_on_chip(k)

    turn = pltpu.make_async_copy(a0t, atr, isem.at[2])
    turn.start()

    @pl.loop(0, T // 256)
    def _(t):
        r = at(t, 256)
        wide = h[r, :].astype(F32)
        scale = lax.rsqrt(jnp.mean(wide * wide, -1, keepdims=True) + 1e-6)
        ct = da[r, :].astype(BF).astype(F32)
        back = scale * ct - wide * (scale * scale * scale * jnp.mean(wide * ct, -1, keepdims=True))
        dh[r, :] = (dh[r, :].astype(F32) + back.astype(BF).astype(F32)).astype(BF)

    start(saved(0))
    turn.wait()

    @pl.loop(0, CHUNKS)
    def _(k):
        n = CHUNKS + k
        slot = n % 2
        wait(weights(0, k, slot, False))
        wait(rows_of(k))

        @pl.when(k < CHUNKS - 1)
        def _():
            start(weights(0, k + 1, 1 - slot, False))
            start(rows_of(k + 1))

        @pl.loop(0, TILES)
        def _(t):
            r = at(t, TILE)
            step = k * TILES + t

            @pl.when(step < CHUNKS * TILES - 1)
            def _():
                start(saved(step + 1))

            dp = dot(dh[r, :], wdv[slot], (1, 1)).astype(BF).astype(F32)
            wait(saved(step))
            du[r, :] = (dp * da[at(step % 2, TILE), pl.ds(0, C)]).astype(BF)
            dg[r, :] = (dp * da[at(2 + step % 2, TILE), pl.ds(0, C)]).astype(BF)

        weight_gradients((k + 1) % 2)
        start(to_near(n))
        finish(k, 1, k)
        sum_on_chip(n)

    @pl.loop(0, CHUNKS)
    def _(k):
        finish(CHUNKS + k, 0, k)

    nsend[...] = jnp.full((8, 128), jnp.sum(ssg[...]) + jnp.sum(ssd[...]), F32)
    norms = [remote(nsend, nrecv.at[i], n_send.at[i], n_recv.at[i], to) for i, to in enumerate((near, far, across))]
    start(norms)

    @pl.loop(0, CHUNKS)
    def _(k):
        wait(results(k, 1, k))
        wait(results(CHUNKS + k, 0, k))

    wait(norms)
    ss[...] = nsend[...] + nrecv[0] + nrecv[1] + nrecv[2]


def backward(*args):
    vmem, sem = pltpu.VMEM, pltpu.SemaphoreType.DMA
    g_rows = 2 * OWN_D
    return pl.pallas_call(
        backward_kernel,
        out_shape=[
            jax.ShapeDtypeStruct((2, OWN_D, FF), BF),
            jax.ShapeDtypeStruct((2, OWN_D, FF), BF),
            jax.ShapeDtypeStruct((2, OWN_F, D), BF),
            jax.ShapeDtypeStruct((8, 128), F32),
        ],
        in_specs=[ANY] * 11,
        out_specs=[ANY] * 3 + [pl.BlockSpec(memory_space=pltpu.VMEM)],
        scratch_shapes=[
            vmem((T, D), BF), vmem((D, T), BF), vmem((T, D), BF), vmem((T, D), BF),
            vmem((2, T, C), BF), vmem((T, C), BF), vmem((T, C), BF), vmem((T, D), F32),
            vmem((2, D, C), BF), vmem((2, D, C), BF), vmem((2, C, D), BF),
            vmem((2, 2, g_rows, C), BF), vmem((2, 2, PIECE, D), BF),
            vmem((2, 2, g_rows, C), BF), vmem((2, 2, PIECE, D), BF),
            vmem((CHUNKS, g_rows, C), BF), vmem((CHUNKS, PIECE, D), BF),
            vmem((2 * CHUNKS, g_rows, C), BF), vmem((2 * CHUNKS, PIECE, D), BF),
            vmem((CHUNKS, g_rows, C), F32), vmem((CHUNKS, PIECE, D), F32),
            vmem((8, C), F32), vmem((8, D), F32), vmem((8, 128), F32), vmem((3, 8, 128), F32),
            sem((4,)), sem((2, 12)), sem((2,)), sem((2, 2)),
            sem((2, 2 * CHUNKS)), sem((2, 2 * CHUNKS)), sem((2, 2 * CHUNKS)), sem((2, 2 * CHUNKS)),
            sem((2 * CHUNKS, 9)), sem((3,)), sem((3,)),
        ],
        compiler_params=pltpu.CompilerParams(vmem_limit_bytes=67_000_000, collective_id=0, has_side_effects=True),
        cost_estimate=pl.CostEstimate(flops=24 * T * D * FF, bytes_accessed=130_000_000, transcendentals=T * FF),
        name="backward",
    )(*args)


def solution(mesh):
    far = [(d, d ^ 2) for d in range(GROUP)]
    near = [(d, d ^ 1) for d in range(GROUP)]

    def step(x, dy, *arrays):
        weights, ms, vs = (arrays[i : i + 3] for i in (0, 3, 6))
        me = lax.axis_index("dp")
        s0, q0, p0, h1, a1, a1t, a0t = forward(x, *weights)
        *gradients, squares = backward(a1, a1t, dy[0], h1, a0t, s0, q0, p0, *weights)
        count = sum(w.size for w in weights)
        factor = jnp.minimum(1.0, 0.5 * lax.rsqrt(squares[0, 0] / count + 1e-30))

        new_w, new_m, new_v = [], [], []
        for w, m, v, g in zip(weights, ms, vs, gradients, strict=True):
            layers, rows, columns = g.shape
            mine = lax.dynamic_index_in_dim(w.reshape(layers, GROUP, rows, columns), me, 1, keepdims=False)

            def adamw(w, m, v, g):
                g = g.astype(F32) * factor
                m = 0.9 * m + 0.1 * g
                v = 0.95 * v + 0.05 * g * g
                return (w.astype(F32) - 0.02 * (m * lax.rsqrt(v + 1e-8) + 0.1 * w.astype(F32))).astype(BF), m, v

            out = jnp.zeros((layers, GROUP, rows, columns), BF)
            for layer in range(layers):
                block = adamw(mine[layer], m[layer], v[layer], g[layer])[0]
                of_far = lax.ppermute(block, "dp", far)
                of_near = lax.ppermute(block, "dp", near)
                of_across = lax.ppermute(of_far, "dp", near)
                for which, part in ((me, block), (me ^ 1, of_near), (me ^ 2, of_far), (me ^ 3, of_across)):
                    out = lax.dynamic_update_slice(out, part[None, None], (layer, which, 0, 0))
            new_w.append(out.reshape(w.shape))
            _, m, v = adamw(mine, m, v, g)
            new_m.append(m)
            new_v.append(v)
        return (*new_w, *new_m, *new_v)

    sequences, whole, rows = P(("rep", "dp")), P(), P(None, "dp")
    return jax.shard_map(
        step,
        mesh=mesh,
        in_specs=(sequences, sequences) + (whole,) * 3 + (rows,) * 6,
        out_specs=(P("rep"),) * 3 + (P("rep", "dp"),) * 6,
        check_vma=False,
    )
```

```python
import jax
import jax.numpy as jnp
from jax import lax
from jax.experimental import pallas as pl
from jax.experimental.pallas import tpu as pltpu
from jax.sharding import PartitionSpec as P


T, D, FF = 2048, 896, 2560
GROUP = 4
OWN_D, OWN_F = D // GROUP, FF // GROUP
CHUNKS, PIECE = 5, 128
C = GROUP * PIECE
TILE = 512
TILES = T // TILE
BF, F32 = jnp.bfloat16, jnp.float32
ANY = pl.BlockSpec(memory_space=pl.ANY)


def dot(a, b, over=(1, 0)):
    return lax.dot_general(a, b, (((over[0],), (over[1],)), ((), ())), preferred_element_type=F32)


def logistic(x):
    return 1.0 / (1.0 + jnp.exp(-x))


def normed(h):
    wide = h.astype(F32)
    return (wide * lax.rsqrt(jnp.mean(wide * wide, -1, keepdims=True) + 1e-6)).astype(BF)


def at(i, size):
    return pl.ds(pl.multiple_of(i * size, size), size)


def hidden(d, k):
    return pl.ds(pl.multiple_of(d * OWN_F + k * PIECE, PIECE), PIECE)


def forward_kernel(x, wg, wu, wd, s_out, q_out, p_out, h_out, a_out, at_out, a0t_out, wgs, wus, wds, p, sem):
    t = pl.program_id(0)

    def copies(k):
        for d in range(GROUP):
            yield pltpu.make_async_copy(wg.at[0, :, hidden(d, k)], wgs.at[k, :, at(d, PIECE)], sem.at[k, d])
            yield pltpu.make_async_copy(wu.at[0, :, hidden(d, k)], wus.at[k, :, at(d, PIECE)], sem.at[k, 4 + d])
        for d in range(GROUP):
            yield pltpu.make_async_copy(wd.at[0, hidden(d, k), :], wds.at[at(k * GROUP + d, PIECE), :], sem.at[k, 8 + d])

    @pl.when(t == 0)
    def _():
        @pl.loop(0, CHUNKS)
        def _(k):
            for c in copies(k):
                c.start()

    a = normed(x[0])
    a0t_out[...] = a.T

    @pl.loop(0, CHUNKS)
    def _(k):
        @pl.when(t == 0)
        def _():
            for c in copies(k):
                c.wait()

        gate = dot(a, wgs[k])
        up = dot(a, wus[k])
        s = logistic(gate)
        silu = gate * s
        prod = (silu * up).astype(BF)
        s_out[k] = silu
        q_out[k] = up * (s * (1.0 + gate * (1.0 - s)))
        p_out[k] = prod
        p[:, at(k, C)] = prod

    h = (x[0].astype(F32) + dot(p[...], wds[...]).astype(BF).astype(F32)).astype(BF)
    h_out[...] = h
    a = normed(h)
    a_out[...] = a
    at_out[...] = a.T


def forward(x, wg, wu, wd):
    wide = jax.ShapeDtypeStruct((CHUNKS, T, C), F32)
    rows = jax.ShapeDtypeStruct((T, D), BF)
    turned = jax.ShapeDtypeStruct((D, T), BF)
    block = pl.BlockSpec((CHUNKS, TILE, C), lambda t: (0, t, 0))
    row_block = pl.BlockSpec((TILE, D), lambda t: (t, 0))
    turned_block = pl.BlockSpec((D, TILE), lambda t: (0, t))
    return pl.pallas_call(
        forward_kernel,
        grid=(TILES,),
        out_shape=[wide, wide, jax.ShapeDtypeStruct((CHUNKS, T, C), BF), rows, rows, turned, turned],
        in_specs=[pl.BlockSpec((1, TILE, D), lambda t: (0, t, 0)), ANY, ANY, ANY],
        out_specs=[block, block, block, row_block, row_block, turned_block, turned_block],
        scratch_shapes=[
            pltpu.VMEM((CHUNKS, D, C), BF),
            pltpu.VMEM((CHUNKS, D, C), BF),
            pltpu.VMEM((FF, D), BF),
            pltpu.VMEM((TILE, FF), BF),
            pltpu.SemaphoreType.DMA((CHUNKS, 12)),
        ],
        compiler_params=pltpu.CompilerParams(vmem_limit_bytes=64_000_000),
        cost_estimate=pl.CostEstimate(flops=6 * T * D * FF, bytes_accessed=80_000_000, transcendentals=T * FF),
        name="forward",
    )(x, wg, wu, wd)


def backward_kernel(
    a1, a1t, dy, h1, a0t, s0, q0, p0, wg, wu, wd,
    gg, gu, gd, ss,
    a, atr, dh, h, pr, dg, du, da, wgv, wuv, wdv, dwg, dwd, rdg, rdd, isg, isd, irg, ird, owng, ownd, ssg, ssd, nsend, nrecv,
    isem, wsem, psem, ssem, d2d_send, d2d_recv, ici_send, ici_recv, osem, n_send, n_recv,
):
    me = lax.axis_index("dp")
    core, chip = me % 2, me // 2
    other = 1 - chip
    near, far, across = me + 1 - 2 * core, (me + 2) % 4, 3 - me

    def remote(src, dst, send, recv, to):
        return pltpu.make_async_remote_copy(src, dst, send, recv, device_id={"dp": to}, device_id_type=pl.DeviceIdType.MESH)

    def weights(layer, k, slot, all_three):
        for d in range(GROUP):
            yield pltpu.make_async_copy(wd.at[layer, hidden(d, k), :], wdv.at[slot, at(d, PIECE), :], wsem.at[slot, d])
        if all_three:
            for d in range(GROUP):
                yield pltpu.make_async_copy(wg.at[layer, :, hidden(d, k)], wgv.at[slot, :, at(d, PIECE)], wsem.at[slot, 4 + d])
                yield pltpu.make_async_copy(wu.at[layer, :, hidden(d, k)], wuv.at[slot, :, at(d, PIECE)], wsem.at[slot, 8 + d])

    def start(copies):
        for c in copies:
            c.start()

    def wait(copies):
        for c in copies:
            c.wait()

    def rows_of(k):
        return [pltpu.make_async_copy(p0.at[k], pr.at[(k + 1) % 2], psem.at[(k + 1) % 2])]

    def saved(step):
        k, t, slot = step // TILES, step % TILES, step % 2
        for i, source in enumerate((s0, q0)):
            yield pltpu.make_async_copy(source.at[k, at(t, TILE), :], da.at[at(2 * i + slot, TILE), pl.ds(0, C)], ssem.at[slot, i])

    first = [pltpu.make_async_copy(src, dst, isem.at[i]) for i, (src, dst) in enumerate(((a1, a), (dy, dh), (a1t, atr), (h1, h)))]
    start(weights(1, 0, 0, True))
    start(first)
    start(rows_of(0))
    barrier = pltpu.get_barrier_semaphore()
    for to in (near, far, across):
        pl.semaphore_signal(barrier, inc=1, device_id={"dp": to}, device_id_type=pl.DeviceIdType.MESH)
    ssg[...] = jnp.zeros_like(ssg)
    ssd[...] = jnp.zeros_like(ssd)

    @pl.loop(0, TILES)
    def _(t):
        da[at(t, TILE), :] = jnp.zeros((TILE, D), F32)

    pl.semaphore_wait(barrier, 3)
    wait(first)

    def weight_gradients(slot):
        @pl.loop(0, 2)
        def _(half):
            down = dot(pr[slot, :, at(half, 2 * PIECE)], dh[...], (0, 0)).astype(BF)
            dwd[1 - core, half] = down[:PIECE]
            dwd[core, half] = down[PIECE:]
            turned = atr[at(half, 2 * OWN_D), :]
            for i, d in enumerate((dg, du)):
                out = dot(turned, d[...]).astype(BF)
                rows = slice(i * OWN_D, (i + 1) * OWN_D)
                dwg[1 - core, half, rows, :] = out[:OWN_D]
                dwg[core, half, rows, :] = out[OWN_D:]

    def to_near(n):
        return [
            remote(dwd.at[0], rdd.at[n % 2], d2d_send.at[0, n], d2d_recv.at[0, n], near),
            remote(dwg.at[0], rdg.at[n % 2], d2d_send.at[1, n], d2d_recv.at[1, n], near),
        ]

    def to_far(n):
        return [
            remote(isd.at[n % CHUNKS], ird.at[n], ici_send.at[0, n], ici_recv.at[0, n], far),
            remote(isg.at[n % CHUNKS], irg.at[n], ici_send.at[1, n], ici_recv.at[1, n], far),
        ]

    def sum_on_chip(n):
        slot, place = n % 2, n % CHUNKS
        near_copies, far_copies = to_near(n), to_far(n)
        for own, got, out, near_copy, far_copy in ((dwd, rdd, isd, near_copies[0], far_copies[0]), (dwg, rdg, isg, near_copies[1], far_copies[1])):
            near_copy.wait()
            out[place] = (own[1, other].astype(F32) + got[slot, other].astype(F32)).astype(BF)
            far_copy.start()
        ownd[place] = dwd[1, chip].astype(F32) + rdd[slot, chip].astype(F32)
        owng[place] = dwg[1, chip].astype(F32) + rdg[slot, chip].astype(F32)

    def results(n, layer, k):
        yield pltpu.make_async_copy(ird.at[n], gd.at[layer, at(k, PIECE), :], osem.at[n, 0])
        for i, out in enumerate((gg, gu)):
            for d in range(GROUP):
                yield pltpu.make_async_copy(
                    irg.at[n, pl.ds(i * OWN_D, OWN_D), at(d, PIECE)], out.at[layer, :, hidden(d, k)], osem.at[n, 1 + i * GROUP + d]
                )

    def finish(n, layer, k):
        place = n % CHUNKS
        for own, got, total, copy in ((ownd, ird, ssd, to_far(n)[0]), (owng, irg, ssg, to_far(n)[1])):
            copy.wait()
            g = (own[place] + got[n].astype(F32)).astype(BF)
            got[n] = g
            g = g.astype(F32)
            total[...] += jnp.sum((g * g).reshape(-1, 8, g.shape[-1]), 0)
        start(results(n, layer, k))

    @pl.loop(0, CHUNKS)
    def _(k):
        slot = k % 2
        wait(weights(1, k, slot, True))

        @pl.when(k < CHUNKS - 1)
        def _():
            start(weights(1, k + 1, 1 - slot, True))

        @pl.when(k == CHUNKS - 1)
        def _():
            start(weights(0, 0, CHUNKS % 2, False))

        @pl.loop(0, TILES)
        def _(t):
            r = at(t, TILE)
            x = a[r, :]
            gate = dot(x, wgv[slot])
            up = dot(x, wuv[slot])
            dp = dot(dh[r, :], wdv[slot], (1, 1)).astype(BF).astype(F32)
            s = logistic(gate)
            silu = gate * s
            pr[0, r, :] = (silu * up).astype(BF)
            dg[r, :] = (dp * (up * (s * (1.0 + gate * (1.0 - s))))).astype(BF)
            du[r, :] = (dp * silu).astype(BF)

        weight_gradients(0)
        start(to_near(k))

        @pl.loop(0, TILES)
        def _(t):
            r = at(t, TILE)
            da[r, :] += dot(dg[r, :], wgv[slot], (1, 1)) + dot(du[r, :], wuv[slot], (1, 1))

        sum_on_chip(k)

    turn = pltpu.make_async_copy(a0t, atr, isem.at[2])
    turn.start()

    @pl.loop(0, T // 256)
    def _(t):
        r = at(t, 256)
        wide = h[r, :].astype(F32)
        scale = lax.rsqrt(jnp.mean(wide * wide, -1, keepdims=True) + 1e-6)
        ct = da[r, :].astype(BF).astype(F32)
        back = scale * ct - wide * (scale * scale * scale * jnp.mean(wide * ct, -1, keepdims=True))
        dh[r, :] = (dh[r, :].astype(F32) + back.astype(BF).astype(F32)).astype(BF)

    start(saved(0))
    turn.wait()

    @pl.loop(0, CHUNKS)
    def _(k):
        n = CHUNKS + k
        slot = n % 2
        wait(weights(0, k, slot, False))
        wait(rows_of(k))

        @pl.when(k < CHUNKS - 1)
        def _():
            start(weights(0, k + 1, 1 - slot, False))
            start(rows_of(k + 1))

        @pl.loop(0, TILES)
        def _(t):
            r = at(t, TILE)
            step = k * TILES + t

            @pl.when(step < CHUNKS * TILES - 1)
            def _():
                start(saved(step + 1))

            dp = dot(dh[r, :], wdv[slot], (1, 1)).astype(BF).astype(F32)
            wait(saved(step))
            du[r, :] = (dp * da[at(step % 2, TILE), pl.ds(0, C)]).astype(BF)
            dg[r, :] = (dp * da[at(2 + step % 2, TILE), pl.ds(0, C)]).astype(BF)

        weight_gradients((k + 1) % 2)
        start(to_near(n))
        finish(k, 1, k)
        sum_on_chip(n)

    @pl.loop(0, CHUNKS)
    def _(k):
        finish(CHUNKS + k, 0, k)

    nsend[...] = jnp.full((8, 128), jnp.sum(ssg[...]) + jnp.sum(ssd[...]), F32)
    norms = [remote(nsend, nrecv.at[i], n_send.at[i], n_recv.at[i], to) for i, to in enumerate((near, far, across))]
    start(norms)

    @pl.loop(0, CHUNKS)
    def _(k):
        wait(results(k, 1, k))
        wait(results(CHUNKS + k, 0, k))

    wait(norms)
    ss[...] = nsend[...] + nrecv[0] + nrecv[1] + nrecv[2]


def backward(*args):
    vmem, sem = pltpu.VMEM, pltpu.SemaphoreType.DMA
    g_rows = 2 * OWN_D
    return pl.pallas_call(
        backward_kernel,
        out_shape=[
            jax.ShapeDtypeStruct((2, OWN_D, FF), BF),
            jax.ShapeDtypeStruct((2, OWN_D, FF), BF),
            jax.ShapeDtypeStruct((2, OWN_F, D), BF),
            jax.ShapeDtypeStruct((8, 128), F32),
        ],
        in_specs=[ANY] * 11,
        out_specs=[ANY] * 3 + [pl.BlockSpec(memory_space=pltpu.VMEM)],
        scratch_shapes=[
            vmem((T, D), BF), vmem((D, T), BF), vmem((T, D), BF), vmem((T, D), BF),
            vmem((2, T, C), BF), vmem((T, C), BF), vmem((T, C), BF), vmem((T, D), F32),
            vmem((2, D, C), BF), vmem((2, D, C), BF), vmem((2, C, D), BF),
            vmem((2, 2, g_rows, C), BF), vmem((2, 2, PIECE, D), BF),
            vmem((2, 2, g_rows, C), BF), vmem((2, 2, PIECE, D), BF),
            vmem((CHUNKS, g_rows, C), BF), vmem((CHUNKS, PIECE, D), BF),
            vmem((2 * CHUNKS, g_rows, C), BF), vmem((2 * CHUNKS, PIECE, D), BF),
            vmem((CHUNKS, g_rows, C), F32), vmem((CHUNKS, PIECE, D), F32),
            vmem((8, C), F32), vmem((8, D), F32), vmem((8, 128), F32), vmem((3, 8, 128), F32),
            sem((4,)), sem((2, 12)), sem((2,)), sem((2, 2)),
            sem((2, 2 * CHUNKS)), sem((2, 2 * CHUNKS)), sem((2, 2 * CHUNKS)), sem((2, 2 * CHUNKS)),
            sem((2 * CHUNKS, 9)), sem((3,)), sem((3,)),
        ],
        compiler_params=pltpu.CompilerParams(vmem_limit_bytes=67_000_000, collective_id=0, has_side_effects=True),
        cost_estimate=pl.CostEstimate(flops=24 * T * D * FF, bytes_accessed=130_000_000, transcendentals=T * FF),
        name="backward",
    )(*args)


def solution(mesh):
    far = [(d, d ^ 2) for d in range(GROUP)]
    near = [(d, d ^ 1) for d in range(GROUP)]

    def step(x, dy, *arrays):
        weights, ms, vs = (arrays[i : i + 3] for i in (0, 3, 6))
        me = lax.axis_index("dp")
        s0, q0, p0, h1, a1, a1t, a0t = forward(x, *weights)
        *gradients, squares = backward(a1, a1t, dy[0], h1, a0t, s0, q0, p0, *weights)
        count = sum(w.size for w in weights)
        factor = jnp.minimum(1.0, 0.5 * lax.rsqrt(squares[0, 0] / count + 1e-30))

        def adamw(w, m, v, g, factor):
            g = g.astype(F32) * factor
            m = 0.9 * m + 0.1 * g
            v = 0.95 * v + 0.05 * g * g
            return (w.astype(F32) - 0.02 * (m * lax.rsqrt(v + 1e-8) + 0.1 * w.astype(F32))).astype(BF), m, v

        mine = []
        for w, g in zip(weights, gradients, strict=True):
            mine.append(lax.dynamic_index_in_dim(w.reshape(g.shape[0], GROUP, *g.shape[1:]), me, 1, keepdims=False))
        units = [(i, layer) for i in range(3) for layer in range(2)]
        blocks = {}
        for i, layer in units:
            block = adamw(mine[i][layer], ms[i][layer], vs[i][layer], gradients[i][layer], factor)[0]
            block, factor = lax.optimization_barrier((block, factor))
            blocks[i, layer] = block
        out = [jnp.zeros((g.shape[0], GROUP, *g.shape[1:]), BF) for g in gradients]
        for i, layer in units:
            block = blocks[i, layer]
            of_far = lax.ppermute(block, "dp", far)
            of_near = lax.ppermute(block, "dp", near)
            of_across = lax.ppermute(of_far, "dp", near)
            for which, part in ((me, block), (me ^ 1, of_near), (me ^ 2, of_far), (me ^ 3, of_across)):
                out[i] = lax.dynamic_update_slice(out[i], part[None, None], (layer, which, 0, 0))
        new_w = [o.reshape(w.shape) for o, w in zip(out, weights, strict=True)]
        new_m, new_v = [], []
        for own, m, v, g in zip(mine, ms, vs, gradients, strict=True):
            _, m, v = adamw(own, m, v, g, factor)
            new_m.append(m)
            new_v.append(v)
        return (*new_w, *new_m, *new_v)

    sequences, whole, rows = P(("rep", "dp")), P(), P(None, "dp")
    return jax.shard_map(
        step,
        mesh=mesh,
        in_specs=(sequences, sequences) + (whole,) * 3 + (rows,) * 6,
        out_specs=(P("rep"),) * 3 + (P("rep", "dp"),) * 6,
        check_vma=False,
    )
```

```python
import jax
import jax.numpy as jnp
from jax import lax
from jax.experimental import pallas as pl
from jax.experimental.pallas import tpu as pltpu
from jax.sharding import PartitionSpec as P


T, D, FF = 2048, 896, 2560
GROUP = 4
OWN_D, OWN_F = D // GROUP, FF // GROUP
CHUNKS, PIECE = 5, 128
C = GROUP * PIECE
SENDS = 3
OWNS = 3
TILE = 512
TILES = T // TILE
BF, F32 = jnp.bfloat16, jnp.float32
ANY = pl.BlockSpec(memory_space=pl.ANY)


def dot(a, b, over=(1, 0)):
    return lax.dot_general(a, b, (((over[0],), (over[1],)), ((), ())), preferred_element_type=F32)


def logistic(x):
    return 1.0 / (1.0 + jnp.exp(-x))


def normed(h):
    wide = h.astype(F32)
    return (wide * lax.rsqrt(jnp.mean(wide * wide, -1, keepdims=True) + 1e-6)).astype(BF)


def at(i, size):
    return pl.ds(pl.multiple_of(i * size, size), size)


def hidden(d, k):
    return pl.ds(pl.multiple_of(d * OWN_F + k * PIECE, PIECE), PIECE)


def step_kernel(
    x, dy, wg, wu, wd,
    gg, gu, gd, ss, s0, q0, p0, a0t,
    a, atr, dh, h, pr, dg, du, da, sq, wgv, wuv, wdv, dwg, dwd, rdg, rdd, isg, isd, irg, ird, owng, ownd, ssg, ssd, nsend, nrecv,
    isem, wsem, psem, ssem, d2d_send, d2d_recv, ici_send, ici_recv, osem, n_send, n_recv,
):
    me = lax.axis_index("dp")
    core, chip = me % 2, me // 2
    other = 1 - chip
    near, far, across = me + 1 - 2 * core, (me + 2) % 4, 3 - me

    def remote(src, dst, send, recv, to):
        return pltpu.make_async_remote_copy(src, dst, send, recv, device_id={"dp": to}, device_id_type=pl.DeviceIdType.MESH)

    def start(copies):
        for c in copies:
            c.start()

    def wait(copies):
        for c in copies:
            c.wait()

    def weights(layer, k, slot, all_three):
        if all_three:
            for d in range(GROUP):
                yield pltpu.make_async_copy(wg.at[layer, :, hidden(d, k)], wgv.at[slot, :, at(d, PIECE)], wsem.at[slot, 4 + d])
                yield pltpu.make_async_copy(wu.at[layer, :, hidden(d, k)], wuv.at[slot, :, at(d, PIECE)], wsem.at[slot, 8 + d])
        for d in range(GROUP):
            yield pltpu.make_async_copy(wd.at[layer, hidden(d, k), :], wdv.at[slot, at(d, PIECE), :], wsem.at[slot, d])

    def product_out(k):
        return pltpu.make_async_copy(pr.at[k % 2], p0.at[k], psem.at[k % 2])

    def product_in(k):
        return pltpu.make_async_copy(p0.at[k], pr.at[(k + 1) % 2], psem.at[(k + 1) % 2])

    def factors_out(step):
        k, t, slot = step // TILES, step % TILES, step % 2
        return [pltpu.make_async_copy(sq.at[slot, i], f.at[k, at(t, TILE), :], ssem.at[slot, i]) for i, f in enumerate((s0, q0))]

    def silu_in(k, t):
        return pltpu.make_async_copy(s0.at[k, at(t, TILE), :], da.at[at(t, TILE), pl.ds(0, C)], ssem.at[0, t])

    def factor_in(k, t):
        return pltpu.make_async_copy(q0.at[k, at(t, TILE), :], sq.at[t // 2, t % 2], ssem.at[1, t])

    first = [pltpu.make_async_copy(src.at[0], dst, isem.at[i]) for i, (src, dst) in enumerate(((x, h), (dy, dh)))]
    start(first)
    start(weights(0, 0, 0, True))
    barrier = pltpu.get_barrier_semaphore()
    for to in (near, far, across):
        pl.semaphore_signal(barrier, inc=1, device_id={"dp": to}, device_id_type=pl.DeviceIdType.MESH)
    ssg[...] = jnp.zeros_like(ssg)
    ssd[...] = jnp.zeros_like(ssd)
    first[0].wait()

    @pl.loop(0, T // 256)
    def _(t):
        r = at(t, 256)
        n = normed(h[r, :])
        a[r, :] = n
        atr[:, r] = n.T
        da[r, :] = jnp.zeros((256, D), F32)

    turned = pltpu.make_async_copy(atr, a0t, isem.at[2])
    turned.start()


    @pl.loop(0, CHUNKS)
    def _(k):
        slot = k % 2
        wait(weights(0, k, slot, True))

        @pl.when(k < CHUNKS - 1)
        def _():
            start(weights(0, k + 1, 1 - slot, True))

        @pl.when(k == CHUNKS - 1)
        def _():
            start(weights(1, 0, 1 - slot, True))

        @pl.when(k >= 2)
        def _():
            product_out(k - 2).wait()

        @pl.loop(0, TILES)
        def _(t):
            r = at(t, TILE)
            step = k * TILES + t
            gate = dot(a[r, :], wgv[slot])
            up = dot(a[r, :], wuv[slot])
            s = logistic(gate)
            silu = gate * s
            prod = (silu * up).astype(BF)
            pr[slot, r, :] = prod
            da[r, :] += dot(prod, wdv[slot])

            @pl.when(step >= 2)
            def _():
                wait(factors_out(step - 2))

            sq[step % 2, 0] = silu
            sq[step % 2, 1] = up * (s * (1.0 + gate * (1.0 - s)))
            start(factors_out(step))

        product_out(k).start()

    first[1].wait()
    turned.wait()

    @pl.loop(0, T // 256)
    def _(t):
        r = at(t, 256)
        out = (h[r, :].astype(F32) + da[r, :].astype(BF).astype(F32)).astype(BF)
        h[r, :] = out
        n = normed(out)
        a[r, :] = n
        atr[:, r] = n.T
        da[r, :] = jnp.zeros((256, D), F32)

    for last in (2, 1):
        product_out(CHUNKS - last).wait()
        wait(factors_out(CHUNKS * TILES - last))
    pl.semaphore_wait(barrier, 3)
    product_in(0).start()

    def to_near(n, part):
        own, got = ((dwd, rdd), (dwg, rdg))[part]
        return remote(own.at[0], got.at[n % 2], d2d_send.at[part, n], d2d_recv.at[part, n], near)

    def to_far(n, part):
        own, got = ((isd, ird), (isg, irg))[part]
        return remote(own.at[n % SENDS], got.at[n], ici_send.at[part, n], ici_recv.at[part, n], far)

    def gradient_down(slot):
        @pl.loop(0, 2, unroll=True)
        def _(half):
            out = dot(pr[slot, :, at(half, 2 * PIECE)], dh[...], (0, 0)).astype(BF)
            dwd[1 - core, half] = out[:PIECE]
            dwd[core, half] = out[PIECE:]

    def gradient(d, i):
        @pl.loop(0, 2, unroll=True)
        def _(half):
            out = dot(atr[at(half, 2 * OWN_D), :], d[...]).astype(BF)
            rows = slice(i * OWN_D, (i + 1) * OWN_D)
            dwg[1 - core, half, rows, :] = out[:OWN_D]
            dwg[core, half, rows, :] = out[OWN_D:]

    def sum_on_chip(n, part):
        slot, place = n % 2, n % OWNS
        own, got, out, kept = ((dwd, rdd, isd, ownd), (dwg, rdg, isg, owng))[part]
        to_near(n, part).wait()

        @pl.when(n >= SENDS)
        def _():
            to_far(n - SENDS, part).wait_send()

        out[n % SENDS] = (own[1, other].astype(F32) + got[slot, other].astype(F32)).astype(BF)
        to_far(n, part).start()
        kept[place] = own[1, chip].astype(F32) + got[slot, chip].astype(F32)

    def gradients(n, slot):
        gradient_down(slot)
        to_near(n, 0).start()
        gradient(dg, 0)
        sum_on_chip(n, 0)
        gradient(du, 1)
        to_near(n, 1).start()

    def results(n):
        layer, k = 1 - n // CHUNKS, n % CHUNKS
        yield pltpu.make_async_copy(ird.at[n], gd.at[layer, at(k, PIECE), :], osem.at[n, 0])
        for i, out in enumerate((gg, gu)):
            for d in range(GROUP):
                yield pltpu.make_async_copy(
                    irg.at[n, pl.ds(i * OWN_D, OWN_D), at(d, PIECE)], out.at[layer, :, hidden(d, k)], osem.at[n, 1 + i * GROUP + d]
                )

    def finish(n):
        place = n % OWNS
        for part, (own, got, total) in enumerate(((ownd, ird, ssd), (owng, irg, ssg))):
            to_far(n, part).wait_recv()
            g = (own[place] + got[n].astype(F32)).astype(BF)
            got[n] = g
            g = g.astype(F32)
            total[...] += jnp.sum((g * g).reshape(-1, 8, g.shape[-1]), 0)
        start(results(n))


    @pl.loop(0, CHUNKS)
    def _(k):
        slot = (CHUNKS + k) % 2
        wait(weights(1, k, slot, True))

        @pl.when(k < CHUNKS - 1)
        def _():
            start(weights(1, k + 1, 1 - slot, True))

        @pl.when(k == CHUNKS - 1)
        def _():
            start(weights(0, 0, 1 - slot, False))

        @pl.loop(0, TILES)
        def _(t):
            r = at(t, TILE)
            n = a[r, :]
            gate = dot(n, wgv[slot])
            up = dot(n, wuv[slot])
            dp = dot(dh[r, :], wdv[slot], (1, 1)).astype(BF).astype(F32)
            s = logistic(gate)
            silu = gate * s
            pr[0, r, :] = (silu * up).astype(BF)
            dg[r, :] = (dp * (up * (s * (1.0 + gate * (1.0 - s))))).astype(BF)
            du[r, :] = (dp * silu).astype(BF)

        @pl.when(k >= OWNS)
        def _():
            finish(k - OWNS)

        gradients(k, 0)

        @pl.loop(0, TILES)
        def _(t):
            r = at(t, TILE)
            da[r, :] += dot(dg[r, :], wgv[slot], (1, 1)) + dot(du[r, :], wuv[slot], (1, 1))

        sum_on_chip(k, 1)

    start(factor_in(0, t) for t in range(TILES))
    turned = pltpu.make_async_copy(a0t, atr, isem.at[2])
    turned.start()

    @pl.loop(0, T // 256)
    def _(t):
        r = at(t, 256)
        wide = h[r, :].astype(F32)
        scale = lax.rsqrt(jnp.mean(wide * wide, -1, keepdims=True) + 1e-6)
        ct = da[r, :].astype(BF).astype(F32)
        back = scale * ct - wide * (scale * scale * scale * jnp.mean(wide * ct, -1, keepdims=True))
        dh[r, :] = (dh[r, :].astype(F32) + back.astype(BF).astype(F32)).astype(BF)

    start(silu_in(0, t) for t in range(TILES))
    turned.wait()


    @pl.loop(0, CHUNKS)
    def _(k):
        n = CHUNKS + k
        slot = k % 2
        wait(weights(0, k, slot, False))
        product_in(k).wait()

        @pl.when(k < CHUNKS - 1)
        def _():
            start(weights(0, k + 1, 1 - slot, False))
            product_in(k + 1).start()

        @pl.loop(0, TILES)
        def _(t):
            r = at(t, TILE)
            silu_in(k, t).wait()
            factor_in(k, t).wait()
            dp = dot(dh[r, :], wdv[slot], (1, 1)).astype(BF).astype(F32)
            du[r, :] = (dp * da[r, pl.ds(0, C)]).astype(BF)
            dg[r, :] = (dp * sq[t // 2, t % 2]).astype(BF)

        @pl.when(k < CHUNKS - 1)
        def _():
            @pl.loop(0, TILES)
            def _(t):
                silu_in(k + 1, t).start()
                factor_in(k + 1, t).start()

        finish(n - OWNS)
        gradients(n, (k + 1) % 2)
        sum_on_chip(n, 1)

    @pl.loop(2 * CHUNKS - OWNS, 2 * CHUNKS)
    def _(n):
        finish(n)

    for last in range(SENDS):
        for part in range(2):
            to_far(2 * CHUNKS - SENDS + last, part).wait_send()

    nsend[...] = jnp.full((8, 128), jnp.sum(ssg[...]) + jnp.sum(ssd[...]), F32)
    norms = [remote(nsend, nrecv.at[i], n_send.at[i], n_recv.at[i], to) for i, to in enumerate((near, far, across))]
    start(norms)

    @pl.loop(0, 2 * CHUNKS)
    def _(n):
        wait(results(n))

    wait(norms)
    ss[...] = nsend[...] + nrecv[0] + nrecv[1] + nrecv[2]


def gradients_of(*args):
    vmem, sem = pltpu.VMEM, pltpu.SemaphoreType.DMA
    g_rows = 2 * OWN_D
    return pl.pallas_call(
        step_kernel,
        out_shape=[
            jax.ShapeDtypeStruct((2, OWN_D, FF), BF),
            jax.ShapeDtypeStruct((2, OWN_D, FF), BF),
            jax.ShapeDtypeStruct((2, OWN_F, D), BF),
            jax.ShapeDtypeStruct((8, 128), F32),
            jax.ShapeDtypeStruct((CHUNKS, T, C), F32),
            jax.ShapeDtypeStruct((CHUNKS, T, C), F32),
            jax.ShapeDtypeStruct((CHUNKS, T, C), BF),
            jax.ShapeDtypeStruct((D, T), BF),
        ],
        in_specs=[ANY] * 5,
        out_specs=[ANY] * 3 + [pl.BlockSpec(memory_space=pltpu.VMEM)] + [ANY] * 4,
        scratch_shapes=[
            vmem((T, D), BF), vmem((D, T), BF), vmem((T, D), BF), vmem((T, D), BF),
            vmem((2, T, C), BF), vmem((T, C), BF), vmem((T, C), BF), vmem((T, D), F32), vmem((2, 2, TILE, C), F32),
            vmem((2, D, C), BF), vmem((2, D, C), BF), vmem((2, C, D), BF),
            vmem((2, 2, g_rows, C), BF), vmem((2, 2, PIECE, D), BF),
            vmem((2, 2, g_rows, C), BF), vmem((2, 2, PIECE, D), BF),
            vmem((SENDS, g_rows, C), BF), vmem((SENDS, PIECE, D), BF),
            vmem((2 * CHUNKS, g_rows, C), BF), vmem((2 * CHUNKS, PIECE, D), BF),
            vmem((OWNS, g_rows, C), F32), vmem((OWNS, PIECE, D), F32),
            vmem((8, C), F32), vmem((8, D), F32), vmem((8, 128), F32), vmem((3, 8, 128), F32),
            sem((3,)), sem((2, 12)), sem((2,)), sem((2, TILES)),
            sem((2, 2 * CHUNKS)), sem((2, 2 * CHUNKS)), sem((2, 2 * CHUNKS)), sem((2, 2 * CHUNKS)),
            sem((2 * CHUNKS, 9)), sem((3,)), sem((3,)),
        ],
        compiler_params=pltpu.CompilerParams(vmem_limit_bytes=67_000_000, collective_id=0, has_side_effects=True),
        cost_estimate=pl.CostEstimate(flops=30 * T * D * FF, bytes_accessed=200_000_000, transcendentals=2 * T * FF),
        name="gradients",
    )(*args)[:4]


def solution(mesh):
    far = [(d, d ^ 2) for d in range(GROUP)]
    near = [(d, d ^ 1) for d in range(GROUP)]

    def step(x, dy, *arrays):
        weights, ms, vs = (arrays[i : i + 3] for i in (0, 3, 6))
        me = lax.axis_index("dp")
        *gradients, squares = gradients_of(x, dy, *weights)
        count = sum(w.size for w in weights)
        factor = jnp.minimum(1.0, 0.5 * lax.rsqrt(squares[0, 0] / count + 1e-30))

        def adamw(w, m, v, g, factor):
            g = g.astype(F32) * factor
            m = 0.9 * m + 0.1 * g
            v = 0.95 * v + 0.05 * g * g
            return (w.astype(F32) - 0.02 * (m * lax.rsqrt(v + 1e-8) + 0.1 * w.astype(F32))).astype(BF), m, v

        mine = []
        for w, g in zip(weights, gradients, strict=True):
            mine.append(lax.dynamic_index_in_dim(w.reshape(g.shape[0], GROUP, *g.shape[1:]), me, 1, keepdims=False))
        units = [(i, layer) for i in range(3) for layer in range(2)]
        blocks = {}
        for i, layer in units:
            block = adamw(mine[i][layer], ms[i][layer], vs[i][layer], gradients[i][layer], factor)[0]
            block, factor = lax.optimization_barrier((block, factor))
            blocks[i, layer] = block
        out = [jnp.zeros((g.shape[0], GROUP, *g.shape[1:]), BF) for g in gradients]
        for i, layer in units:
            block = blocks[i, layer]
            of_far = lax.ppermute(block, "dp", far)
            of_near = lax.ppermute(block, "dp", near)
            of_across = lax.ppermute(of_far, "dp", near)
            for which, part in ((me, block), (me ^ 1, of_near), (me ^ 2, of_far), (me ^ 3, of_across)):
                out[i] = lax.dynamic_update_slice(out[i], part[None, None], (layer, which, 0, 0))
        new_w = [o.reshape(w.shape) for o, w in zip(out, weights, strict=True)]
        new_m, new_v = [], []
        for own, m, v, g in zip(mine, ms, vs, gradients, strict=True):
            _, m, v = adamw(own, m, v, g, factor)
            new_m.append(m)
            new_v.append(v)
        return (*new_w, *new_m, *new_v)

    sequences, whole, rows = P(("rep", "dp")), P(), P(None, "dp")
    return jax.shard_map(
        step,
        mesh=mesh,
        in_specs=(sequences, sequences) + (whole,) * 3 + (rows,) * 6,
        out_specs=(P("rep"),) * 3 + (P("rep", "dp"),) * 6,
        check_vma=False,
    )
```

```python
import functools

import jax
import jax.numpy as jnp
from jax import lax
from jax.experimental import pallas as pl
from jax.experimental.pallas import tpu as pltpu
from jax.sharding import PartitionSpec as P


T, D, FF = 2048, 896, 2560
GROUP = 4
OWN_D, OWN_F = D // GROUP, FF // GROUP
CHUNKS, PIECE = 5, 128
C = GROUP * PIECE
SENDS = 3
OWNS = 3
TILE = 512
TILES = T // TILE
BF, F32 = jnp.bfloat16, jnp.float32
ANY = pl.BlockSpec(memory_space=pl.ANY)


def dot(a, b, over=(1, 0)):
    return lax.dot_general(a, b, (((over[0],), (over[1],)), ((), ())), preferred_element_type=F32)


def logistic(x):
    return 1.0 / (1.0 + jnp.exp(-x))


def normed(h):
    wide = h.astype(F32)
    return (wide * lax.rsqrt(jnp.mean(wide * wide, -1, keepdims=True) + 1e-6)).astype(BF)


def at(i, size):
    return pl.ds(pl.multiple_of(i * size, size), size)


def hidden(d, k):
    return pl.ds(pl.multiple_of(d * OWN_F + k * PIECE, PIECE), PIECE)


def step_kernel(
    x, dy, wg, wu, wd,
    gg, gu, gd, ss, s0, q0, p0, a0t,
    a, atr, dh, h, pr, dgu, da, sq, wgu, wdv, dwg, dwd, rdg, rdd, isg, isd, irg, ird, owng, ownd, ssg, ssd, nsend, nrecv,
    isem, wsem, psem, ssem, d2d_send, d2d_recv, ici_send, ici_recv, osem, n_send, n_recv,
):
    me = lax.axis_index("dp")
    core, chip = me % 2, me // 2
    other = 1 - chip
    near, far, across = me + 1 - 2 * core, (me + 2) % 4, 3 - me

    def remote(src, dst, send, recv, to):
        return pltpu.make_async_remote_copy(src, dst, send, recv, device_id={"dp": to}, device_id_type=pl.DeviceIdType.MESH)

    def start(copies):
        for c in copies:
            c.start()

    def wait(copies):
        for c in copies:
            c.wait()

    def weights(layer, k, slot, all_three):
        if all_three:
            for d in range(GROUP):
                yield pltpu.make_async_copy(wg.at[layer, :, hidden(d, k)], wgu.at[slot, :, pl.ds(d * PIECE, PIECE)], wsem.at[slot, 4 + d])
                yield pltpu.make_async_copy(wu.at[layer, :, hidden(d, k)], wgu.at[slot, :, pl.ds(C + d * PIECE, PIECE)], wsem.at[slot, 8 + d])
        for d in range(GROUP):
            yield pltpu.make_async_copy(wd.at[layer, hidden(d, k), :], wdv.at[slot, at(d, PIECE), :], wsem.at[slot, d])

    def product_out(k):
        return pltpu.make_async_copy(pr.at[k % 2], p0.at[k], psem.at[k % 2])

    def product_in(k):
        return pltpu.make_async_copy(p0.at[k], pr.at[(k + 1) % 2], psem.at[(k + 1) % 2])

    def factors_out(step):
        k, t, slot = step // TILES, step % TILES, step % 2
        return [pltpu.make_async_copy(sq.at[slot, i], f.at[k, at(t, TILE), :], ssem.at[slot, i]) for i, f in enumerate((s0, q0))]

    def silu_in(k, t):
        return pltpu.make_async_copy(s0.at[k, at(t, TILE), :], da.at[at(t, TILE), pl.ds(0, C)], ssem.at[0, t])

    def factor_in(k, t):
        return pltpu.make_async_copy(q0.at[k, at(t, TILE), :], sq.at[t // 2, t % 2], ssem.at[1, t])

    first = [pltpu.make_async_copy(src.at[0], dst, isem.at[i]) for i, (src, dst) in enumerate(((x, h), (dy, dh)))]
    start(first)
    start(weights(0, 0, 0, True))
    barrier = pltpu.get_barrier_semaphore()
    for to in (near, far, across):
        pl.semaphore_signal(barrier, inc=1, device_id={"dp": to}, device_id_type=pl.DeviceIdType.MESH)
    ssg[...] = jnp.zeros_like(ssg)
    ssd[...] = jnp.zeros_like(ssd)
    first[0].wait()

    @pl.loop(0, T // 256)
    def _(t):
        r = at(t, 256)
        n = normed(h[r, :])
        a[r, :] = n
        atr[:, r] = n.T
        da[r, :] = jnp.zeros((256, D), F32)

    turned = pltpu.make_async_copy(atr, a0t, isem.at[2])
    turned.start()


    @pl.loop(0, CHUNKS)
    def _(k):
        slot = k % 2
        wait(weights(0, k, slot, True))

        @pl.when(k < CHUNKS - 1)
        def _():
            start(weights(0, k + 1, 1 - slot, True))

        @pl.when(k == CHUNKS - 1)
        def _():
            start(weights(1, 0, 1 - slot, True))

        @pl.when(k >= 2)
        def _():
            product_out(k - 2).wait()

        @pl.loop(0, TILES)
        def _(t):
            r = at(t, TILE)
            step = k * TILES + t
            wide = dot(a[r, :], wgu[slot])
            gate, up = wide[:, :C], wide[:, C:]
            s = logistic(gate)
            silu = gate * s
            prod = (silu * up).astype(BF)
            pr[slot, r, :] = prod
            da[r, :] += dot(prod, wdv[slot])

            @pl.when(step >= 2)
            def _():
                wait(factors_out(step - 2))

            sq[step % 2, 0] = silu
            sq[step % 2, 1] = up * (s * (1.0 + gate * (1.0 - s)))
            start(factors_out(step))

        product_out(k).start()

    first[1].wait()
    turned.wait()

    @pl.loop(0, T // 256)
    def _(t):
        r = at(t, 256)
        out = (h[r, :].astype(F32) + da[r, :].astype(BF).astype(F32)).astype(BF)
        h[r, :] = out
        n = normed(out)
        a[r, :] = n
        atr[:, r] = n.T
        da[r, :] = jnp.zeros((256, D), F32)

    for last in (2, 1):
        product_out(CHUNKS - last).wait()
        wait(factors_out(CHUNKS * TILES - last))
    pl.semaphore_wait(barrier, 3)
    product_in(0).start()

    def to_near(n, part):
        own, got = ((dwd, rdd), (dwg, rdg))[part]
        return remote(own.at[0], got.at[n % 2], d2d_send.at[part, n], d2d_recv.at[part, n], near)

    def to_far(n, part):
        own, got = ((isd, ird), (isg, irg))[part]
        return remote(own.at[n % SENDS], got.at[n], ici_send.at[part, n], ici_recv.at[part, n], far)

    def gradient_down(slot):
        @pl.loop(0, 2, unroll=True)
        def _(half):
            out = dot(pr[slot, :, at(half, 2 * PIECE)], dh[...], (0, 0)).astype(BF)
            dwd[1 - core, half] = out[:PIECE]
            dwd[core, half] = out[PIECE:]

    def gradient_wide(half):
        out = dot(atr[half * 2 * OWN_D : (half + 1) * 2 * OWN_D, :], dgu[...]).astype(BF)
        for q, where in enumerate((1 - core, core)):
            for i in range(2):
                dwg[where, half, i * OWN_D : (i + 1) * OWN_D, :] = out[q * OWN_D : (q + 1) * OWN_D, i * C : (i + 1) * C]

    def sum_on_chip(n, part):
        slot, place = n % 2, n % OWNS
        own, got, out, kept = ((dwd, rdd, isd, ownd), (dwg, rdg, isg, owng))[part]
        to_near(n, part).wait()

        @pl.when(n >= SENDS)
        def _():
            to_far(n - SENDS, part).wait_send()

        out[n % SENDS] = (own[1, other].astype(F32) + got[slot, other].astype(F32)).astype(BF)
        to_far(n, part).start()
        kept[place] = own[1, chip].astype(F32) + got[slot, chip].astype(F32)

    def gradients(n, slot):
        gradient_down(slot)
        to_near(n, 0).start()
        gradient_wide(0)
        sum_on_chip(n, 0)
        gradient_wide(1)
        to_near(n, 1).start()

    def results(n):
        layer, k = 1 - n // CHUNKS, n % CHUNKS
        yield pltpu.make_async_copy(ird.at[n], gd.at[layer, at(k, PIECE), :], osem.at[n, 0])
        for i, out in enumerate((gg, gu)):
            for d in range(GROUP):
                yield pltpu.make_async_copy(
                    irg.at[n, pl.ds(i * OWN_D, OWN_D), at(d, PIECE)], out.at[layer, :, hidden(d, k)], osem.at[n, 1 + i * GROUP + d]
                )

    def finish(n):
        place = n % OWNS
        for part, (own, got, total) in enumerate(((ownd, ird, ssd), (owng, irg, ssg))):
            to_far(n, part).wait_recv()
            g = (own[place] + got[n].astype(F32)).astype(BF)
            got[n] = g
            g = g.astype(F32)
            total[...] += jnp.sum((g * g).reshape(-1, 8, g.shape[-1]), 0)
        start(results(n))


    @pl.loop(0, CHUNKS)
    def _(k):
        slot = (CHUNKS + k) % 2
        wait(weights(1, k, slot, True))

        @pl.when(k < CHUNKS - 1)
        def _():
            start(weights(1, k + 1, 1 - slot, True))

        @pl.when(k == CHUNKS - 1)
        def _():
            start(weights(0, 0, 1 - slot, False))

        @pl.loop(0, TILES)
        def _(t):
            r = at(t, TILE)
            wide = dot(a[r, :], wgu[slot])
            gate, up = wide[:, :C], wide[:, C:]
            dp = dot(dh[r, :], wdv[slot], (1, 1)).astype(BF).astype(F32)
            s = logistic(gate)
            silu = gate * s
            pr[0, r, :] = (silu * up).astype(BF)
            dgu[r, pl.ds(0, C)] = (dp * (up * (s * (1.0 + gate * (1.0 - s))))).astype(BF)
            dgu[r, pl.ds(C, C)] = (dp * silu).astype(BF)

        @pl.when(k >= OWNS)
        def _():
            finish(k - OWNS)

        gradients(k, 0)

        @pl.loop(0, TILES)
        def _(t):
            r = at(t, TILE)
            da[r, :] += dot(dgu[r, :], wgu[slot], (1, 1))

        sum_on_chip(k, 1)

    start(factor_in(0, t) for t in range(TILES))
    turned = pltpu.make_async_copy(a0t, atr, isem.at[2])
    turned.start()

    @pl.loop(0, T // 256)
    def _(t):
        r = at(t, 256)
        wide = h[r, :].astype(F32)
        scale = lax.rsqrt(jnp.mean(wide * wide, -1, keepdims=True) + 1e-6)
        ct = da[r, :].astype(BF).astype(F32)
        back = scale * ct - wide * (scale * scale * scale * jnp.mean(wide * ct, -1, keepdims=True))
        dh[r, :] = (dh[r, :].astype(F32) + back.astype(BF).astype(F32)).astype(BF)

    start(silu_in(0, t) for t in range(TILES))
    turned.wait()


    @pl.loop(0, CHUNKS)
    def _(k):
        n = CHUNKS + k
        slot = k % 2
        wait(weights(0, k, slot, False))
        product_in(k).wait()

        @pl.when(k < CHUNKS - 1)
        def _():
            start(weights(0, k + 1, 1 - slot, False))
            product_in(k + 1).start()

        @pl.loop(0, TILES)
        def _(t):
            r = at(t, TILE)
            silu_in(k, t).wait()
            factor_in(k, t).wait()
            dp = dot(dh[r, :], wdv[slot], (1, 1)).astype(BF).astype(F32)
            dgu[r, pl.ds(C, C)] = (dp * da[r, pl.ds(0, C)]).astype(BF)
            dgu[r, pl.ds(0, C)] = (dp * sq[t // 2, t % 2]).astype(BF)

        @pl.when(k < CHUNKS - 1)
        def _():
            @pl.loop(0, TILES)
            def _(t):
                silu_in(k + 1, t).start()
                factor_in(k + 1, t).start()

        finish(n - OWNS)
        gradients(n, (k + 1) % 2)
        sum_on_chip(n, 1)

    @pl.loop(2 * CHUNKS - OWNS, 2 * CHUNKS)
    def _(n):
        finish(n)

    for last in range(SENDS):
        for part in range(2):
            to_far(2 * CHUNKS - SENDS + last, part).wait_send()

    nsend[...] = jnp.full((8, 128), jnp.sum(ssg[...]) + jnp.sum(ssd[...]), F32)
    norms = [remote(nsend, nrecv.at[i], n_send.at[i], n_recv.at[i], to) for i, to in enumerate((near, far, across))]
    start(norms)

    @pl.loop(0, 2 * CHUNKS)
    def _(n):
        wait(results(n))

    wait(norms)
    squares = nsend[...] + nrecv[0] + nrecv[1] + nrecv[2]
    factor = jnp.minimum(1.0, 0.5 * lax.rsqrt(squares / (6 * D * FF) + 1e-30))
    for i in range(FF // 128):
        ss[:, i * 128 : (i + 1) * 128] = factor


def gradients_of(*args):
    vmem, sem = pltpu.VMEM, pltpu.SemaphoreType.DMA
    g_rows = 2 * OWN_D
    return pl.pallas_call(
        step_kernel,
        out_shape=[
            jax.ShapeDtypeStruct((2, OWN_D, FF), BF),
            jax.ShapeDtypeStruct((2, OWN_D, FF), BF),
            jax.ShapeDtypeStruct((2, OWN_F, D), BF),
            jax.ShapeDtypeStruct((8, FF), F32),
            jax.ShapeDtypeStruct((CHUNKS, T, C), F32),
            jax.ShapeDtypeStruct((CHUNKS, T, C), F32),
            jax.ShapeDtypeStruct((CHUNKS, T, C), BF),
            jax.ShapeDtypeStruct((D, T), BF),
        ],
        in_specs=[ANY] * 5,
        out_specs=[ANY] * 3 + [pl.BlockSpec(memory_space=pltpu.VMEM)] + [ANY] * 4,
        scratch_shapes=[
            vmem((T, D), BF), vmem((D, T), BF), vmem((T, D), BF), vmem((T, D), BF),
            vmem((2, T, C), BF), vmem((T, 2 * C), BF), vmem((T, D), F32), vmem((2, 2, TILE, C), F32),
            vmem((2, D, 2 * C), BF), vmem((2, C, D), BF),
            vmem((2, 2, g_rows, C), BF), vmem((2, 2, PIECE, D), BF),
            vmem((2, 2, g_rows, C), BF), vmem((2, 2, PIECE, D), BF),
            vmem((SENDS, g_rows, C), BF), vmem((SENDS, PIECE, D), BF),
            vmem((2 * CHUNKS, g_rows, C), BF), vmem((2 * CHUNKS, PIECE, D), BF),
            vmem((OWNS, g_rows, C), F32), vmem((OWNS, PIECE, D), F32),
            vmem((8, C), F32), vmem((8, D), F32), vmem((8, 128), F32), vmem((3, 8, 128), F32),
            sem((3,)), sem((2, 12)), sem((2,)), sem((2, TILES)),
            sem((2, 2 * CHUNKS)), sem((2, 2 * CHUNKS)), sem((2, 2 * CHUNKS)), sem((2, 2 * CHUNKS)),
            sem((2 * CHUNKS, 9)), sem((3,)), sem((3,)),
        ],
        compiler_params=pltpu.CompilerParams(vmem_limit_bytes=67_000_000, collective_id=0, has_side_effects=True),
        cost_estimate=pl.CostEstimate(flops=30 * T * D * FF, bytes_accessed=200_000_000, transcendentals=2 * T * FF),
        name="gradients",
    )(*args)[:4]


def places(shapes):
    space = pl.BlockSpec(memory_space=pltpu.HBM)
    return list(pl.pallas_call(lambda *_: None, out_shape=[jax.ShapeDtypeStruct(s, BF) for s in shapes], out_specs=[space] * len(shapes), name="places")())


def place_kernel(layer, which, part, _, out, tile, sem):
    me = lax.axis_index("dp")
    block = (me, me + 1 - 2 * (me % 2), (me + 2) % 4, 3 - me)[which]
    rows = part.shape[0] // 4
    ins = [pltpu.make_async_copy(part.at[pl.ds(i * rows, rows)], tile.at[pl.ds(i * rows, rows)], sem.at[0, i]) for i in range(4)]
    outs = [pltpu.make_async_copy(tile.at[pl.ds(i * rows, rows)], out.at[layer, block, pl.ds(i * rows, rows)], sem.at[1, i]) for i in range(4)]
    for c in ins:
        c.start()
    for i, o in zip(ins, outs, strict=True):
        i.wait()
        o.start()
    for c in outs:
        c.wait()


def place(out, part, layer, which):
    space = pl.BlockSpec(memory_space=pltpu.HBM)
    return pl.pallas_call(
        functools.partial(place_kernel, layer, which),
        out_shape=jax.ShapeDtypeStruct(out.shape, out.dtype),
        in_specs=[ANY, space],
        out_specs=space,
        scratch_shapes=[pltpu.VMEM(part.shape, part.dtype), pltpu.SemaphoreType.DMA((2, 4))],
        input_output_aliases={1: 0},
        cost_estimate=pl.CostEstimate(flops=part.size, bytes_accessed=4 * part.size, transcendentals=0),
        name="place",
    )(part, out)


def solution(mesh):
    far = [(d, d ^ 2) for d in range(GROUP)]
    near = [(d, d ^ 1) for d in range(GROUP)]

    def step(x, dy, *arrays):
        weights, ms, vs = (arrays[i : i + 3] for i in (0, 3, 6))
        me = lax.axis_index("dp")
        *gradients, factors = gradients_of(x, dy, *weights)

        def adamw(w, m, v, g, factor):
            g = g.astype(F32) * factor[:1, : g.shape[-1]]
            m = 0.9 * m + 0.1 * g
            v = 0.95 * v + 0.05 * g * g
            return (w.astype(F32) - 0.02 * (m * lax.rsqrt(v + 1e-8) + 0.1 * w.astype(F32))).astype(BF), m, v

        units = [(0, 0, 0, 112), (0, 0, 112, 112)] + [(i, layer, 0, gradients[i].shape[1]) for i in range(3) for layer in range(2)][1:]
        blocks = {}
        for u, (i, layer, first, rows) in enumerate(units):
            g = gradients[i]
            whole = weights[i].reshape(g.shape[0], GROUP, *g.shape[1:])
            w = lax.dynamic_slice(whole, (layer, me, first, 0), (1, 1, rows, g.shape[2]))[0, 0]
            block = adamw(w, *(t[i][layer, first : first + rows] for t in (ms, vs, gradients)), factors)[0]
            block, factors = lax.optimization_barrier((block, factors))
            blocks[u] = block
        out = places([(g.shape[0], GROUP, *g.shape[1:]) for g in gradients])
        for u, (i, layer, first, rows) in enumerate(units):
            block = blocks[u]
            of_far = lax.ppermute(block, "dp", far)
            of_near = lax.ppermute(block, "dp", near)
            of_across = lax.ppermute(of_far, "dp", near)
            for which, part in enumerate((block, of_near, of_far, of_across)):
                if i == 2:
                    out[i] = place(out[i], part, layer, which)
                else:
                    out[i] = lax.dynamic_update_slice(out[i], part[None, None], (layer, me ^ which, first, 0))
        new_w = [o.reshape(w.shape) for o, w in zip(out, weights, strict=True)]
        new_m, new_v = [], []
        for m, v, g in zip(ms, vs, gradients, strict=True):
            _, m, v = adamw(jnp.zeros((), BF), m, v, g, factors)
            new_m.append(m)
            new_v.append(v)
        return (*new_w, *new_m, *new_v)

    sequences, whole, rows = P(("rep", "dp")), P(), P(None, "dp")
    return jax.shard_map(
        step,
        mesh=mesh,
        in_specs=(sequences, sequences) + (whole,) * 3 + (rows,) * 6,
        out_specs=(P("rep"),) * 3 + (P("rep", "dp"),) * 6,
        check_vma=False,
    )
```

```python
import functools

import jax
import jax.numpy as jnp
from jax import lax
from jax.experimental import pallas as pl
from jax.experimental.pallas import tpu as pltpu
from jax.sharding import PartitionSpec as P


T, D, FF = 2048, 896, 2560
GROUP = 4
OWN_D, OWN_F = D // GROUP, FF // GROUP
CHUNKS, PIECE = 5, 128
C = GROUP * PIECE
SENDS = 3
OWNS = 3
TILE = 512
TILES = T // TILE
BF, F32 = jnp.bfloat16, jnp.float32
ANY = pl.BlockSpec(memory_space=pl.ANY)


def dot(a, b, over=(1, 0)):
    return lax.dot_general(a, b, (((over[0],), (over[1],)), ((), ())), preferred_element_type=F32)


def logistic(x):
    return 1.0 / (1.0 + jnp.exp(-x))


def normed(h):
    wide = h.astype(F32)
    return (wide * lax.rsqrt(jnp.mean(wide * wide, -1, keepdims=True) + 1e-6)).astype(BF)


def at(i, size):
    return pl.ds(pl.multiple_of(i * size, size), size)


def hidden(d, k):
    return pl.ds(pl.multiple_of(d * OWN_F + k * PIECE, PIECE), PIECE)


def step_kernel(
    x, dy, wg, wu, wd,
    gg, gu, gd, ss, s0, q0, p0, a0t,
    a, atr, dh, h, pr, dgu, da, sq, wgu, wdv, dwg, dwd, rdg, rdd, isg, isd, irg, ird, owng, ownd, ssg, ssd, nsend, nrecv,
    isem, xsem, wsem, psem, ssem, d2d_send, d2d_recv, ici_send, ici_recv, osem, n_send, n_recv,
):
    me = lax.axis_index("dp")
    core, chip = me % 2, me // 2
    other = 1 - chip
    near, far, across = me + 1 - 2 * core, (me + 2) % 4, 3 - me

    def remote(src, dst, send, recv, to):
        return pltpu.make_async_remote_copy(src, dst, send, recv, device_id={"dp": to}, device_id_type=pl.DeviceIdType.MESH)

    def start(copies):
        for c in copies:
            c.start()

    def wait(copies):
        for c in copies:
            c.wait()

    def weights(layer, k, slot, all_three):
        if all_three:
            for d in range(GROUP):
                yield pltpu.make_async_copy(wg.at[layer, :, hidden(d, k)], wgu.at[slot, :, pl.ds(d * PIECE, PIECE)], wsem.at[slot, 4 + d])
                yield pltpu.make_async_copy(wu.at[layer, :, hidden(d, k)], wgu.at[slot, :, pl.ds(C + d * PIECE, PIECE)], wsem.at[slot, 8 + d])
        for d in range(GROUP):
            yield pltpu.make_async_copy(wd.at[layer, hidden(d, k), :], wdv.at[slot, at(d, PIECE), :], wsem.at[slot, d])

    def product_out(k):
        return pltpu.make_async_copy(pr.at[k % 2], p0.at[k], psem.at[k % 2])

    def product_in(k):
        return pltpu.make_async_copy(p0.at[k], pr.at[(k + 1) % 2], psem.at[(k + 1) % 2])

    def factors_out(step):
        k, t, slot = step // TILES, step % TILES, step % 2
        return [pltpu.make_async_copy(sq.at[slot, i], f.at[k, at(t, TILE), :], ssem.at[slot, i]) for i, f in enumerate((s0, q0))]

    def silu_in(k, t):
        return pltpu.make_async_copy(s0.at[k, at(t, TILE), :], da.at[at(t, TILE), pl.ds(0, C)], ssem.at[0, t])

    def factor_in(k, t):
        return pltpu.make_async_copy(q0.at[k, at(t, TILE), :], sq.at[t // 2, t % 2], ssem.at[1, t])

    def x_in(t):
        return pltpu.make_async_copy(x.at[0, at(t, 256), :], h.at[at(t, 256), :], xsem.at[t])

    start(x_in(t) for t in range(T // 256))
    start(weights(0, 0, 0, True))
    dy_in = pltpu.make_async_copy(dy.at[0], dh, isem.at[1])
    dy_in.start()
    barrier = pltpu.get_barrier_semaphore()
    for to in (near, far, across):
        pl.semaphore_signal(barrier, inc=1, device_id={"dp": to}, device_id_type=pl.DeviceIdType.MESH)
    ssg[...] = jnp.zeros_like(ssg)
    ssd[...] = jnp.zeros_like(ssd)

    @pl.loop(0, T // 256)
    def _(t):
        r = at(t, 256)
        x_in(t).wait()
        n = normed(h[r, :])
        a[r, :] = n
        atr[:, r] = n.T
        da[r, :] = jnp.zeros((256, D), F32)

    turned = pltpu.make_async_copy(atr, a0t, isem.at[2])
    turned.start()


    @pl.loop(0, CHUNKS)
    def _(k):
        slot = k % 2
        wait(weights(0, k, slot, True))

        @pl.when(k < CHUNKS - 1)
        def _():
            start(weights(0, k + 1, 1 - slot, True))

        @pl.when(k == CHUNKS - 1)
        def _():
            start(weights(1, 0, 1 - slot, True))

        @pl.when(k >= 2)
        def _():
            product_out(k - 2).wait()

        @pl.loop(0, TILES)
        def _(t):
            r = at(t, TILE)
            step = k * TILES + t
            wide = dot(a[r, :], wgu[slot])
            gate, up = wide[:, :C], wide[:, C:]
            s = logistic(gate)
            silu = gate * s
            prod = (silu * up).astype(BF)
            pr[slot, r, :] = prod
            da[r, :] += dot(prod, wdv[slot])

            @pl.when(step >= 2)
            def _():
                wait(factors_out(step - 2))

            sq[step % 2, 0] = silu
            sq[step % 2, 1] = up * (s * (1.0 + gate * (1.0 - s)))
            start(factors_out(step))

        product_out(k).start()

    dy_in.wait()
    turned.wait()

    @pl.loop(0, T // 256)
    def _(t):
        r = at(t, 256)
        out = (h[r, :].astype(F32) + da[r, :].astype(BF).astype(F32)).astype(BF)
        h[r, :] = out
        n = normed(out)
        a[r, :] = n
        atr[:, r] = n.T
        da[r, :] = jnp.zeros((256, D), F32)

    for last in (2, 1):
        product_out(CHUNKS - last).wait()
        wait(factors_out(CHUNKS * TILES - last))
    pl.semaphore_wait(barrier, 3)
    product_in(0).start()

    def to_near(n, part):
        own, got = ((dwd, rdd), (dwg, rdg))[part]
        return remote(own.at[0], got.at[n % 2], d2d_send.at[part, n], d2d_recv.at[part, n], near)

    def to_far(n, part):
        own, got = ((isd, ird), (isg, irg))[part]
        return remote(own.at[n % SENDS], got.at[n], ici_send.at[part, n], ici_recv.at[part, n], far)

    def gradient_down(slot):
        @pl.loop(0, 2, unroll=True)
        def _(half):
            out = dot(pr[slot, :, at(half, 2 * PIECE)], dh[...], (0, 0)).astype(BF)
            dwd[1 - core, half] = out[:PIECE]
            dwd[core, half] = out[PIECE:]

    def gradient_wide(half):
        out = dot(atr[half * 2 * OWN_D : (half + 1) * 2 * OWN_D, :], dgu[...]).astype(BF)
        for q, where in enumerate((1 - core, core)):
            for i in range(2):
                dwg[where, half, i * OWN_D : (i + 1) * OWN_D, :] = out[q * OWN_D : (q + 1) * OWN_D, i * C : (i + 1) * C]

    def sum_on_chip(n, part):
        slot, place = n % 2, n % OWNS
        own, got, out, kept = ((dwd, rdd, isd, ownd), (dwg, rdg, isg, owng))[part]
        to_near(n, part).wait()

        @pl.when(n >= SENDS)
        def _():
            to_far(n - SENDS, part).wait_send()

        out[n % SENDS] = (own[1, other].astype(F32) + got[slot, other].astype(F32)).astype(BF)
        to_far(n, part).start()
        kept[place] = own[1, chip].astype(F32) + got[slot, chip].astype(F32)

    def gradients(n, slot):
        gradient_down(slot)
        to_near(n, 0).start()

        @pl.when(n >= OWNS)
        def _():
            finish(n - OWNS)

        gradient_wide(0)
        sum_on_chip(n, 0)
        gradient_wide(1)
        to_near(n, 1).start()

    def results(n):
        layer, k = 1 - n // CHUNKS, n % CHUNKS
        yield pltpu.make_async_copy(ird.at[n], gd.at[layer, at(k, PIECE), :], osem.at[n, 0])
        for i, out in enumerate((gg, gu)):
            for d in range(GROUP):
                yield pltpu.make_async_copy(
                    irg.at[n, pl.ds(i * OWN_D, OWN_D), at(d, PIECE)], out.at[layer, :, hidden(d, k)], osem.at[n, 1 + i * GROUP + d]
                )

    def finish(n):
        place = n % OWNS
        for part, (own, got, total) in enumerate(((ownd, ird, ssd), (owng, irg, ssg))):
            to_far(n, part).wait_recv()
            g = (own[place] + got[n].astype(F32)).astype(BF)
            got[n] = g
            g = g.astype(F32)
            total[...] += jnp.sum((g * g).reshape(-1, 8, g.shape[-1]), 0)
        start(results(n))


    @pl.loop(0, CHUNKS)
    def _(k):
        slot = (CHUNKS + k) % 2
        wait(weights(1, k, slot, True))

        @pl.when(k < CHUNKS - 1)
        def _():
            start(weights(1, k + 1, 1 - slot, True))

        @pl.when(k == CHUNKS - 1)
        def _():
            start(weights(0, 0, 1 - slot, False))

        @pl.loop(0, TILES)
        def _(t):
            r = at(t, TILE)
            wide = dot(a[r, :], wgu[slot])
            gate, up = wide[:, :C], wide[:, C:]
            dp = dot(dh[r, :], wdv[slot], (1, 1)).astype(BF).astype(F32)
            s = logistic(gate)
            silu = gate * s
            pr[0, r, :] = (silu * up).astype(BF)
            dgu[r, pl.ds(0, C)] = (dp * (up * (s * (1.0 + gate * (1.0 - s))))).astype(BF)
            dgu[r, pl.ds(C, C)] = (dp * silu).astype(BF)

        gradients(k, 0)

        @pl.loop(0, TILES)
        def _(t):
            r = at(t, TILE)
            da[r, :] += dot(dgu[r, :], wgu[slot], (1, 1))

        sum_on_chip(k, 1)

    start(factor_in(0, t) for t in range(TILES))
    turned = pltpu.make_async_copy(a0t, atr, isem.at[2])
    turned.start()

    @pl.loop(0, TILES)
    def _(t):
        for i in range(TILE // 256):
            r = pl.ds(pl.multiple_of(t * TILE + i * 256, 256), 256)
            wide = h[r, :].astype(F32)
            scale = lax.rsqrt(jnp.mean(wide * wide, -1, keepdims=True) + 1e-6)
            ct = da[r, :].astype(BF).astype(F32)
            back = scale * ct - wide * (scale * scale * scale * jnp.mean(wide * ct, -1, keepdims=True))
            dh[r, :] = (dh[r, :].astype(F32) + back.astype(BF).astype(F32)).astype(BF)
        silu_in(0, t).start()

    turned.wait()


    @pl.loop(0, CHUNKS)
    def _(k):
        n = CHUNKS + k
        slot = k % 2
        wait(weights(0, k, slot, False))
        product_in(k).wait()

        @pl.when(k < CHUNKS - 1)
        def _():
            start(weights(0, k + 1, 1 - slot, False))
            product_in(k + 1).start()

        @pl.loop(0, TILES)
        def _(t):
            r = at(t, TILE)
            silu_in(k, t).wait()
            factor_in(k, t).wait()
            dp = dot(dh[r, :], wdv[slot], (1, 1)).astype(BF).astype(F32)
            dgu[r, pl.ds(C, C)] = (dp * da[r, pl.ds(0, C)]).astype(BF)
            dgu[r, pl.ds(0, C)] = (dp * sq[t // 2, t % 2]).astype(BF)

        @pl.when(k < CHUNKS - 1)
        def _():
            @pl.loop(0, TILES)
            def _(t):
                silu_in(k + 1, t).start()
                factor_in(k + 1, t).start()

        gradients(n, (k + 1) % 2)
        sum_on_chip(n, 1)

    @pl.loop(2 * CHUNKS - OWNS, 2 * CHUNKS)
    def _(n):
        finish(n)

    for last in range(SENDS):
        for part in range(2):
            to_far(2 * CHUNKS - SENDS + last, part).wait_send()

    nsend[...] = jnp.full((8, 128), jnp.sum(ssg[...]) + jnp.sum(ssd[...]), F32)
    norms = [remote(nsend, nrecv.at[i], n_send.at[i], n_recv.at[i], to) for i, to in enumerate((near, far, across))]
    start(norms)

    @pl.loop(0, 2 * CHUNKS)
    def _(n):
        wait(results(n))

    wait(norms)
    squares = nsend[...] + nrecv[0] + nrecv[1] + nrecv[2]
    factor = jnp.minimum(1.0, 0.5 * lax.rsqrt(squares / (6 * D * FF) + 1e-30))
    for i in range(FF // 128):
        ss[:, i * 128 : (i + 1) * 128] = factor


def gradients_of(*args):
    vmem, sem = pltpu.VMEM, pltpu.SemaphoreType.DMA
    g_rows = 2 * OWN_D
    return pl.pallas_call(
        step_kernel,
        out_shape=[
            jax.ShapeDtypeStruct((2, OWN_D, FF), BF),
            jax.ShapeDtypeStruct((2, OWN_D, FF), BF),
            jax.ShapeDtypeStruct((2, OWN_F, D), BF),
            jax.ShapeDtypeStruct((8, FF), F32),
            jax.ShapeDtypeStruct((CHUNKS, T, C), F32),
            jax.ShapeDtypeStruct((CHUNKS, T, C), F32),
            jax.ShapeDtypeStruct((CHUNKS, T, C), BF),
            jax.ShapeDtypeStruct((D, T), BF),
        ],
        in_specs=[ANY] * 5,
        out_specs=[ANY] * 3 + [pl.BlockSpec(memory_space=pltpu.VMEM)] + [ANY] * 4,
        scratch_shapes=[
            vmem((T, D), BF), vmem((D, T), BF), vmem((T, D), BF), vmem((T, D), BF),
            vmem((2, T, C), BF), vmem((T, 2 * C), BF), vmem((T, D), F32), vmem((2, 2, TILE, C), F32),
            vmem((2, D, 2 * C), BF), vmem((2, C, D), BF),
            vmem((2, 2, g_rows, C), BF), vmem((2, 2, PIECE, D), BF),
            vmem((2, 2, g_rows, C), BF), vmem((2, 2, PIECE, D), BF),
            vmem((SENDS, g_rows, C), BF), vmem((SENDS, PIECE, D), BF),
            vmem((2 * CHUNKS, g_rows, C), BF), vmem((2 * CHUNKS, PIECE, D), BF),
            vmem((OWNS, g_rows, C), F32), vmem((OWNS, PIECE, D), F32),
            vmem((8, C), F32), vmem((8, D), F32), vmem((8, 128), F32), vmem((3, 8, 128), F32),
            sem((3,)), sem((T // 256,)), sem((2, 12)), sem((2,)), sem((2, TILES)),
            sem((2, 2 * CHUNKS)), sem((2, 2 * CHUNKS)), sem((2, 2 * CHUNKS)), sem((2, 2 * CHUNKS)),
            sem((2 * CHUNKS, 9)), sem((3,)), sem((3,)),
        ],
        compiler_params=pltpu.CompilerParams(vmem_limit_bytes=67_000_000, collective_id=0, has_side_effects=True),
        cost_estimate=pl.CostEstimate(flops=30 * T * D * FF, bytes_accessed=200_000_000, transcendentals=2 * T * FF),
        name="gradients",
    )(*args)[:4]


def places(shapes):
    space = pl.BlockSpec(memory_space=pltpu.HBM)
    return list(pl.pallas_call(lambda *_: None, out_shape=[jax.ShapeDtypeStruct(s, BF) for s in shapes], out_specs=[space] * len(shapes), name="places")())


def place_kernel(layer, which, first, part, _, out, tile, sem):
    me = lax.axis_index("dp")
    block = (me, me + 1 - 2 * (me % 2), (me + 2) % 4, 3 - me)[which]
    rows = part.shape[0] // 4
    ins = [pltpu.make_async_copy(part.at[pl.ds(i * rows, rows)], tile.at[pl.ds(i * rows, rows)], sem.at[0, i]) for i in range(4)]
    outs = [pltpu.make_async_copy(tile.at[pl.ds(i * rows, rows)], out.at[layer, block, pl.ds(first + i * rows, rows)], sem.at[1, i]) for i in range(4)]
    for c in ins:
        c.start()
    for i, o in zip(ins, outs, strict=True):
        i.wait()
        o.start()
    for c in outs:
        c.wait()


def place(out, part, layer, which, first):
    space = pl.BlockSpec(memory_space=pltpu.HBM)
    return pl.pallas_call(
        functools.partial(place_kernel, layer, which, first),
        out_shape=jax.ShapeDtypeStruct(out.shape, out.dtype),
        in_specs=[ANY, space],
        out_specs=space,
        scratch_shapes=[pltpu.VMEM(part.shape, part.dtype), pltpu.SemaphoreType.DMA((2, 4))],
        input_output_aliases={1: 0},
        cost_estimate=pl.CostEstimate(flops=part.size, bytes_accessed=4 * part.size, transcendentals=0),
        name="place",
    )(part, out)


def solution(mesh):
    far = [(d, d ^ 2) for d in range(GROUP)]
    near = [(d, d ^ 1) for d in range(GROUP)]

    def step(x, dy, *arrays):
        weights, ms, vs = (arrays[i : i + 3] for i in (0, 3, 6))
        me = lax.axis_index("dp")
        *gradients, factors = gradients_of(x, dy, *weights)

        def adamw(w, m, v, g, factor):
            g = g.astype(F32) * factor[:1, : g.shape[-1]]
            m = 0.9 * m + 0.1 * g
            v = 0.95 * v + 0.05 * g * g
            return (w.astype(F32) - 0.02 * (m * lax.rsqrt(v + 1e-8) + 0.1 * w.astype(F32))).astype(BF), m, v

        units = [(0, 0, 0, 112), (0, 0, 112, 112)] + [(i, layer, 0, gradients[i].shape[1]) for i in range(3) for layer in range(2)][1:-1]
        units += [(2, 1, 0, OWN_F // 2), (2, 1, OWN_F // 2, OWN_F // 2)]
        blocks = {}
        for u, (i, layer, first, rows) in enumerate(units):
            g = gradients[i]
            whole = weights[i].reshape(g.shape[0], GROUP, *g.shape[1:])
            w = lax.dynamic_slice(whole, (layer, me, first, 0), (1, 1, rows, g.shape[2]))[0, 0]
            block = adamw(w, *(t[i][layer, first : first + rows] for t in (ms, vs, gradients)), factors)[0]
            block, factors = lax.optimization_barrier((block, factors))
            blocks[u] = block
        out = places([(g.shape[0], GROUP, *g.shape[1:]) for g in gradients])
        for u, (i, layer, first, rows) in enumerate(units):
            block = blocks[u]
            of_far = lax.ppermute(block, "dp", far)
            of_near = lax.ppermute(block, "dp", near)
            of_across = lax.ppermute(of_far, "dp", near)
            for which, part in enumerate((block, of_near, of_far, of_across)):
                if i == 2:
                    out[i] = place(out[i], part, layer, which, first)
                else:
                    out[i] = lax.dynamic_update_slice(out[i], part[None, None], (layer, me ^ which, first, 0))
        new_w = [o.reshape(w.shape) for o, w in zip(out, weights, strict=True)]
        new_m, new_v = [], []
        for m, v, g in zip(ms, vs, gradients, strict=True):
            _, m, v = adamw(jnp.zeros((), BF), m, v, g, factors)
            new_m.append(m)
            new_v.append(v)
        return (*new_w, *new_m, *new_v)

    sequences, whole, rows = P(("rep", "dp")), P(), P(None, "dp")
    return jax.shard_map(
        step,
        mesh=mesh,
        in_specs=(sequences, sequences) + (whole,) * 3 + (rows,) * 6,
        out_specs=(P("rep"),) * 3 + (P("rep", "dp"),) * 6,
        check_vma=False,
    )
```
